256 devices in a mesh: row: 4 (over y_lo, core), blk: 64 (over y_hi, x, z).
Axes of the slice: x: 4, y: 4 (y_hi: 2, y_lo: 2; y = y_hi * 2 + y_lo), z: 8, core: 2. Of those that a mesh axis runs over, the one named last changes fastest.
Arguments:
- matrix: float32 [16384, 16384], P('row', 'blk'), may hold values from -6 to 6
Outputs:
- rotated: float32 [16384, 16384], P('row', 'blk')
- off_measure: float32 [2], replicated
The draws below stay inside these ranges and needn't reach their ends.
All inputs are finite; a program needn't handle non-finite values.
Results may differ from the reference program's by a relative error of at most 0.00012.
Values sent between devices are 32-bit elements; how exact they have to be, the bound alone decides.
No kernel may reach another device: no remote copies, remote signals or barrier semaphores. Data moves between devices by JAX's collectives and lax.ppermute only.
A program may use at most 64 MiB of HBM per device.

```python
import jax
import jax.numpy as jnp
from jax import lax

B = 128
STEPS = 2
NS_ITERS = 4
ROWS = 16384
NCOLS = 16384
N_BLK = 64


def levels(own_key, extent, cuts, least, largest):
    def one(dim, parts):
        draws = jax.random.uniform(jax.random.fold_in(jax.random.fold_in(own_key, 6), dim), (parts,), jnp.float32, least / len(cuts), largest / len(cuts))
        return jnp.repeat(jnp.exp(draws), extent[dim] // parts).reshape((-1,) + (1,) * (len(extent) - dim - 1))

    factor_of = one(*cuts[0])
    for cut in cuts[1:]:
        factor_of = factor_of * one(*cut)
    return factor_of


def bell_draw(stream_key, shape, spread, reach, split=(), kind=jnp.bfloat16):
    entries = jax.random.normal(stream_key, shape, jnp.float32) * spread
    if len(split) > 0:
        entries = levels(stream_key, shape, split, -0.22, 0.18) * entries
    return jnp.clip(entries, min=-reach, max=reach).astype(kind)


def setup_inputs(seed: int = 0) -> dict:
    streams_of = jax.random.split(jax.random.key(seed), 2)
    return {
        "matrix": bell_draw(streams_of[0], (ROWS, NCOLS), 1.0, 6.0, ((0, 4), (1, 64)), jnp.float32),
    }


HIGH = lax.Precision.HIGHEST

def inverse_root(square, bound_scale):
    identity = jnp.eye(square.shape[0], dtype=jnp.float32)
    current = square / bound_scale
    result = identity
    for count_index in range(NS_ITERS):
        factor = 1.5 * identity - 0.5 * jnp.dot(result, current, precision=HIGH)
        current = jnp.dot(current, factor, precision=HIGH)
        result = jnp.dot(factor, result, precision=HIGH)
    return result / jnp.sqrt(bound_scale)

def reference(matrix):
    blocks = matrix.reshape(ROWS, N_BLK, 2, B)
    left_block = blocks[:, :, 0]
    right_block = blocks[:, :, 1]
    identity = jnp.eye(B, dtype=jnp.float32)
    norm_list = []
    for step_index in range(STEPS):
        cross_gram = jnp.einsum('rpi,rpj->pij', left_block, right_block, precision=HIGH)
        first_norms = lax.optimization_barrier(jnp.sum(left_block * left_block, axis=0))
        second_norms = lax.optimization_barrier(jnp.sum(right_block * right_block, axis=0))
        cosines = cross_gram * lax.rsqrt(first_norms)[:, :, None] * lax.rsqrt(second_norms)[:, None, :]
        norm_list.append(jnp.mean(lax.optimization_barrier(jnp.sum(cosines * cosines, axis=(1, 2)))))
        coupling = 0.5 * cosines
        bound_scale = 1.0 + lax.optimization_barrier(jnp.sum(coupling * coupling, axis=(1, 2)))
        first_square = identity + jnp.einsum('pij,pkj->pik', coupling, coupling, precision=HIGH)
        second_square = identity + jnp.einsum('pji,pjk->pik', coupling, coupling, precision=HIGH)
        first_root = jax.vmap(inverse_root)(first_square, bound_scale)
        second_root = jax.vmap(inverse_root)(second_square, bound_scale)
        mixed_left = left_block - jnp.einsum('rpj,pij->rpi', right_block, coupling, precision=HIGH)
        mixed_right = right_block + jnp.einsum('rpi,pij->rpj', left_block, coupling, precision=HIGH)
        new_left = jnp.einsum('rpi,pij->rpj', mixed_left, first_root, precision=HIGH)
        new_right = jnp.einsum('rpi,pij->rpj', mixed_right, second_root, precision=HIGH)
        if step_index % 2 == 0:
            left_block = jnp.roll(new_left, 1, axis=1)
            right_block = new_right
        else:
            left_block = new_left
            right_block = jnp.roll(new_right, 1, axis=1)
    rotated = jnp.stack([left_block, right_block], axis=2).reshape(ROWS, 2 * B * N_BLK)
    return (rotated, jnp.stack(norm_list))
```

```python
import functools

import jax
import jax.numpy as jnp
from jax import lax
from jax.experimental import pallas as pl
from jax.experimental.pallas import tpu as pltpu
from jax.sharding import PartitionSpec as P

STEPS = 2
NS_ITERS = 4
B = 128
PACK = 136
UNITS = 32
FRONT = (4, 4, 4, 4, 4, 2)
BACK = (5, 5)
TILE = 128

VM = pl.BlockSpec(memory_space=pltpu.VMEM)
ANY = pl.BlockSpec(memory_space=pl.ANY)
F32 = jnp.float32
BF16 = jnp.bfloat16


def params(mib=24):
    return pltpu.CompilerParams(vmem_limit_bytes=mib * 1024 * 1024)


def cost(flops, moved):
    return pl.CostEstimate(flops=int(flops), bytes_accessed=int(moved), transcendentals=0)


def halves(x):
    high = x.astype(BF16)
    low = (x - high.astype(F32)).astype(BF16)
    return high, low


def dot(a, b):
    return jnp.dot(a, b, preferred_element_type=F32)


def dot_rows(a, b):
    return lax.dot_general(a, b, (((0,), (0,)), ((), ())), preferred_element_type=F32)


def split_dot(a, b):
    ah, al = a
    bh, bl = b
    return dot(ah, bh) + (dot(ah, bl) + dot(al, bh))


def gram_tile(left, right):
    lh, ll = halves(left)
    rh, rl = halves(right)
    full = dot_rows(jnp.concatenate([lh, ll], 1), jnp.concatenate([rh, rl], 1))
    return (full[:B, :B] + full[B:, B:]) + (full[:B, B:] + full[B:, :B])


def column_squares(x):
    return jnp.sum((x * x).reshape(x.shape[0] // 8, 8, x.shape[1]), axis=0)


def gram_body(blocks, m_ref, o_ref, c_acc, n_acc):
    step = pl.program_id(0)

    @pl.when(step == 0)
    def _():
        c_acc[...] = jnp.zeros_like(c_acc)
        n_acc[...] = jnp.zeros_like(n_acc)

    x = m_ref[...]
    n_acc[...] += column_squares(x)
    c_acc[...] += gram_tile(x[:, :B], x[:, B:])

    @pl.when(step == blocks - 1)
    def _():
        norms = jnp.sum(n_acc[...], axis=0, keepdims=True)
        o_ref[:B, :] = c_acc[...]
        o_ref[B:, :] = jnp.concatenate(
            [norms[:, :B], norms[:, B:], jnp.zeros((PACK - B - 2, B), F32)], axis=0
        )


def first_gram(matrix):
    rows = matrix.shape[0]
    block = rows // 8
    return pl.pallas_call(
        functools.partial(gram_body, 8),
        grid=(8,),
        in_specs=[pl.BlockSpec((block, 2 * B), lambda i: (i, 0))],
        out_specs=pl.BlockSpec((PACK, B), lambda i: (0, 0)),
        out_shape=jax.ShapeDtypeStruct((PACK, B), F32),
        scratch_shapes=[pltpu.VMEM((B, B), F32), pltpu.VMEM((8, 2 * B), F32)],
        compiler_params=params(16),
        cost_estimate=cost(rows * B * B * 8, rows * B * 8),
        name="first_gram",
    )(matrix)


def root_body(a_ref, b_ref, c_ref, d_ref, wh_ref, wl_ref, s_ref):
    total = (a_ref[...] + b_ref[...]) + (c_ref[...] + d_ref[...])
    inverse = lax.rsqrt(total[B : B + 8, :])
    first = jnp.broadcast_to(inverse[0:1, :], (B, B)).T
    cosines = total[:B, :] * first * inverse[1:2, :]
    squares = jnp.sum(cosines * cosines)
    k = 0.5 * cosines
    scale = 1.0 + jnp.sum(k * k)
    kt = k.T
    row = lax.broadcasted_iota(jnp.int32, (B, B), 0)
    col = lax.broadcasted_iota(jnp.int32, (B, B), 1)
    eye = (row == col).astype(F32)
    ks, kts = halves(k), halves(kt)
    current = [(eye + split_dot(ks, kts)) / scale, (eye + split_dot(kts, ks)) / scale]
    result = [None, None]
    for step in range(NS_ITERS):
        for side in range(2):
            ys = halves(current[side])
            if step == 0:
                factor = 1.5 * eye - 0.5 * current[side]
                fs = halves(factor)
                result[side] = factor
            else:
                zs = halves(result[side])
                factor = 1.5 * eye - 0.5 * split_dot(zs, ys)
                fs = halves(factor)
                result[side] = split_dot(fs, zs)
            if step < NS_ITERS - 1:
                current[side] = split_dot(ys, fs)
    root = lax.sqrt(jnp.full((1, B), scale, F32))
    q1 = result[0] / root
    q2 = result[1] / root
    q1s, q2s = halves(q1), halves(q2)
    corner = split_dot(ks, q2s)
    lower = -split_dot(kts, q1s)
    for value, rows, cols in ((q1, 0, 0), (corner, 0, B), (lower, B, 0), (q2, B, B)):
        high, low = halves(value)
        wh_ref[rows : rows + B, cols : cols + B] = high
        wl_ref[rows : rows + B, cols : cols + B] = low
    s_ref[...] = jnp.full((8, B), squares, F32)


def roots(parts):
    return pl.pallas_call(
        root_body,
        in_specs=[VM] * 4,
        out_specs=[VM] * 3,
        out_shape=[
            jax.ShapeDtypeStruct((2 * B, 2 * B), BF16),
            jax.ShapeDtypeStruct((2 * B, 2 * B), BF16),
            jax.ShapeDtypeStruct((8, B), F32),
        ],
        compiler_params=params(8),
        cost_estimate=cost(30e6, 1e6),
        name="roots",
    )(*parts)


def mixed(x, wh, wl):
    xh, xl = halves(x)
    return dot(xh, wh) + (dot(xh, wl) + dot(xl, wh))


def update_body(start, sizes, want_left, want_right, m_ref, wh_ref, wl_ref, *outs):
    lo = 0 if want_left else B
    hi = 2 * B if want_right else B
    wh, wl = wh_ref[:, lo:hi], wl_ref[:, lo:hi]
    outs = list(outs)
    at = start
    for size in sizes:
        lefts = outs.pop(0) if want_left else None
        rights = outs.pop(0) if want_right else None

        def tile(i, _, at=at, lefts=lefts, rights=rights):
            rows = pl.ds(pl.multiple_of(i * TILE, TILE), TILE)
            source = pl.ds(pl.multiple_of(at + i * TILE, TILE), TILE)
            value = mixed(m_ref[source, :], wh, wl)
            if lefts is not None:
                lefts[rows, :] = value[:, :B]
            if rights is not None:
                rights[rows, :] = value[:, value.shape[1] - B :]
            return 0

        lax.fori_loop(0, size // TILE, tile, 0)
        at += size


def update(matrix, w, start, sizes, want_left, want_right, name):
    shapes = []
    for size in sizes:
        shapes += [jax.ShapeDtypeStruct((size, B), F32)] * (want_left + want_right)
    total = sum(sizes)
    lead = start
    return pl.pallas_call(
        functools.partial(update_body, lead, sizes, want_left, want_right),
        in_specs=[VM] * 3,
        out_specs=[VM] * len(shapes),
        out_shape=shapes,
        compiler_params=params(24),
        cost_estimate=cost(6 * total * 256 * B * len(shapes) / len(sizes), total * B * 16),
        name=name,
    )(matrix, *w)


def partial_body(count, starts, with_right, has_base, *refs):
    lefts = refs[:count]
    right = refs[count]
    base = refs[count + 1] if has_base else None
    o_ref = refs[-1]
    acc = jnp.zeros((B, B), F32)
    lsq = jnp.zeros((8, B), F32)
    rsq = jnp.zeros((8, B), F32)
    for left, start in zip(lefts, starts):
        size = left.shape[0]

        def tile(i, carry, left=left, start=start):
            a, l, r = carry
            x = left[pl.ds(pl.multiple_of(i * TILE, TILE), TILE), :]
            y = right[pl.ds(pl.multiple_of(start + i * TILE, TILE), TILE), :]
            a = a + gram_tile(x, y)
            l = l + column_squares(x)
            if with_right:
                r = r + column_squares(y)
            return a, l, r

        acc, lsq, rsq = lax.fori_loop(0, size // TILE, tile, (acc, lsq, rsq))
    tail = jnp.concatenate(
        [
            jnp.sum(lsq, axis=0, keepdims=True),
            jnp.sum(rsq, axis=0, keepdims=True),
            jnp.zeros((PACK - B - 2, B), F32),
        ],
        axis=0,
    )
    if has_base:
        acc = acc + base[:B, :]
        tail = tail + base[B:, :]
    o_ref[:B, :] = acc
    o_ref[B:, :] = tail


def partial(lefts, starts, right, with_right, base, name):
    total = sum(x.shape[0] for x in lefts)
    operands = [*lefts, right] + ([base] if base is not None else [])
    return pl.pallas_call(
        functools.partial(partial_body, len(lefts), starts, with_right, base is not None),
        in_specs=[VM] * len(operands),
        out_specs=VM,
        out_shape=jax.ShapeDtypeStruct((PACK, B), F32),
        compiler_params=params(16),
        cost_estimate=cost(total * B * B * 8, total * B * 8),
        name=name,
    )(*operands)


def add_squares_body(x_ref, base_ref, o_ref):
    def tile(i, r):
        return r + column_squares(x_ref[pl.ds(pl.multiple_of(i * TILE, TILE), TILE), :])

    squares = lax.fori_loop(0, x_ref.shape[0] // TILE, tile, jnp.zeros((8, B), F32))
    line = jnp.sum(squares, axis=0, keepdims=True)
    where = lax.broadcasted_iota(jnp.int32, (PACK - B, B), 0)
    o_ref[:B, :] = base_ref[:B, :]
    o_ref[B:, :] = base_ref[B:, :] + jnp.where(where == 1, line, 0.0)


def add_squares(x, base):
    return pl.pallas_call(
        add_squares_body,
        in_specs=[VM] * 2,
        out_specs=VM,
        out_shape=jax.ShapeDtypeStruct((PACK, B), F32),
        compiler_params=params(16),
        cost_estimate=cost(x.size, x.size * 4),
        name="add_squares",
    )(x, base)


def second_body(starts, firsts, rows0, aliased, *refs):
    count = len(starts)
    xs = refs[:count]
    r_ref, wh_ref, wl_ref = refs[count : count + 3]
    rest = refs[count + 3 + (1 if aliased else 0) :]
    out = rest[0]
    ys = rest[1 : 1 + count]
    held, sem = rest[1 + count :]
    wh, wl = wh_ref[...], wl_ref[...]
    for x, y, start, first in zip(xs, ys, starts, firsts):

        def tile(i, _, x=x, y=y, start=start, first=first):
            here = pl.ds(pl.multiple_of(i * TILE, TILE), TILE)
            other = pl.ds(pl.multiple_of(start + i * TILE, TILE), TILE)
            both = jnp.concatenate([x[here, :], r_ref[other, :]], axis=1)
            value = mixed(both, wh, wl)
            held[pl.ds(pl.multiple_of(first + i * TILE, TILE), TILE), :] = value[:, :B]
            y[here, :] = value[:, B:]
            return 0

        lax.fori_loop(0, x.shape[0] // TILE, tile, 0)
    copy = pltpu.make_async_copy(
        held, out.at[pl.ds(rows0, held.shape[0]), pl.ds(0, B)], sem
    )
    copy.start()
    copy.wait()


def second(xs, right, starts, w, out, rows, rows0, name):
    firsts, at = [], 0
    for x in xs:
        firsts.append(at)
        at += x.shape[0]
    shapes = [jax.ShapeDtypeStruct((rows, 2 * B), F32)] + [
        jax.ShapeDtypeStruct(x.shape, F32) for x in xs
    ]
    operands = [*xs, right, *w] + ([out] if out is not None else [])
    specs = [VM] * (len(xs) + 3) + ([ANY] if out is not None else [])
    return pl.pallas_call(
        functools.partial(second_body, tuple(starts), tuple(firsts), rows0, out is not None),
        in_specs=specs,
        out_specs=[ANY] + [VM] * len(xs),
        out_shape=shapes,
        scratch_shapes=[pltpu.VMEM((at, B), F32), pltpu.SemaphoreType.DMA],
        input_output_aliases={} if out is None else {len(operands) - 1: 0},
        compiler_params=params(24),
        cost_estimate=cost(6 * at * 256 * 256, at * B * 20),
        name=name,
    )(*operands)


def place_body(starts, *refs):
    count = len(starts)
    ys = refs[:count]
    out = refs[count + 1]
    sems = refs[count + 2]
    copies = []
    for n, (y, start) in enumerate(zip(ys, starts)):
        copies.append(
            pltpu.make_async_copy(
                y, out.at[pl.ds(start, y.shape[0]), pl.ds(B, B)], sems.at[n]
            )
        )
    for copy in copies:
        copy.start()
    for copy in copies:
        copy.wait()


def place(ys, starts, out, name):
    return pl.pallas_call(
        functools.partial(place_body, tuple(starts)),
        in_specs=[ANY] * (len(ys) + 1),
        out_specs=ANY,
        out_shape=jax.ShapeDtypeStruct(out.shape, F32),
        scratch_shapes=[pltpu.SemaphoreType.DMA((len(ys),))],
        input_output_aliases={len(ys): 0},
        compiler_params=params(8),
        cost_estimate=cost(1, sum(y.size for y in ys) * 8),
        name=name,
    )(*ys, out)


def shifted(value, steps):
    count = lax.axis_size("blk")
    return lax.ppermute(value, "blk", [(s, (s + steps) % count) for s in range(count)])


def of_group(value):
    count = lax.axis_size("row")
    parts = [value]
    for mask in range(1, count):
        parts.append(lax.ppermute(value, "row", [(s, s ^ mask) for s in range(count)]))
    return parts


def sum_over_pairs(value):
    peers = lax.axis_size("blk")
    everything = lax.all_to_all(
        jnp.broadcast_to(value[None], (peers, *value.shape)), "blk", 0, 0, tiled=True
    )
    return jnp.sum(everything, axis=0)


def on_device(matrix):
    rows = matrix.shape[0]
    unit = rows // UNITS
    front = [n * unit for n in FRONT]
    back = [n * unit for n in BACK]
    front_rows, back_rows = sum(front), sum(back)
    front_at = [sum(front[:i]) for i in range(len(front))]
    back_at = [sum(back[:i]) for i in range(len(back))]

    wh, wl, squares0 = roots(of_group(first_gram(matrix)))
    w = (wh, wl)
    (x0,) = update(matrix, w, 0, [front[0]], True, False, "update_a")
    got = [shifted(x0, 1)]
    (right_back,) = update(matrix, w, front_rows, [back_rows], False, True, "update_b")
    behind = shifted(right_back, -1)
    xs = update(matrix, w, front[0], front[1:], True, False, "update_c")
    got += [shifted(x, 1) for x in xs]
    xb = update(matrix, w, front_rows, back, True, False, "update_d")
    (right_front,) = update(matrix, w, 0, [front_rows], False, True, "update_e")

    helped = partial(xb, back_at, behind, False, None, "partial_back")
    helped = shifted(helped, 1)
    got_back = [shifted(x, 1) for x in xb]

    sums = add_squares(right_back, helped)
    cut = len(got) - 2
    sums = partial(got[:cut], front_at[:cut], right_front, True, sums, "partial_a")
    sums = partial(got[cut:], front_at[cut:], right_front, True, sums, "partial_b")
    wh, wl, squares1 = roots(of_group(sums))
    w = (wh, wl)

    out, *ys = second(got, right_front, front_at, w, None, rows, 0, "second_a")
    out, *yb = second(got_back, right_back, back_at, w, out, rows, front_rows, "second_b")
    arrived = [shifted(y, 1) for y in [*ys, *yb]]
    totals = sum_over_pairs(jnp.stack([squares0[0, 0], squares1[0, 0]]))
    off_measure = totals / float(lax.axis_size("blk"))
    places = front_at + [front_rows + a for a in back_at]
    out = place(arrived, places, out, "place")
    return out, off_measure


def solution(mesh):
    return jax.shard_map(
        on_device,
        mesh=mesh,
        in_specs=(P("row", "blk"),),
        out_specs=(P("row", "blk"), P()),
        check_vma=False,
    )
```

```python
import functools

import jax
import jax.numpy as jnp
from jax import lax
from jax.experimental import pallas as pl
from jax.experimental.pallas import tpu as pltpu
from jax.sharding import PartitionSpec as P


STEPS = 2
NS_ITERS = 4
B = 128
PACK = 136
UNITS = 32
FRONT = (2, 4, 4, 4, 4, 4)
BACK = (5, 5)

VM = pl.BlockSpec(memory_space=pltpu.VMEM)
ANY = pl.BlockSpec(memory_space=pl.ANY)
HBM = pl.BlockSpec(memory_space=pltpu.HBM)
F32 = jnp.float32
BF16 = jnp.bfloat16


def params(mib=24):
    return pltpu.CompilerParams(vmem_limit_bytes=mib * 1024 * 1024)


def cost(flops, moved):
    return pl.CostEstimate(flops=int(flops), bytes_accessed=int(moved), transcendentals=0)


def halves(x):
    high = x.astype(BF16)
    low = (x - high.astype(F32)).astype(BF16)
    return high, low


def dot(a, b):
    return jnp.dot(a, b, preferred_element_type=F32)


def dot_rows(a, b):
    return lax.dot_general(a, b, (((0,), (0,)), ((), ())), preferred_element_type=F32)


def split_dot(a, b):
    ah, al = a
    bh, bl = b
    return dot(ah, bh) + (dot(ah, bl) + dot(al, bh))


def gram_tile(left, right):
    lh, ll = halves(left)
    rh, rl = halves(right)
    full = dot_rows(jnp.concatenate([lh, ll], 1), jnp.concatenate([rh, rl], 1))
    return (full[:B, :B] + full[B:, B:]) + (full[:B, B:] + full[B:, :B])


def column_squares(x):
    return jnp.sum((x * x).reshape(x.shape[0] // 8, 8, x.shape[1]), axis=0)


def gram_body(blocks, m_ref, o_ref, held_ref, c_acc, n_acc, sems):
    block = m_ref.shape[0] // blocks

    def load(i):
        rows = pl.ds(i * block, block)
        return pltpu.make_async_copy(m_ref.at[rows, :], held_ref.at[rows, :], sems.at[i])

    for i in range(blocks):
        load(i).start()
    for i in range(blocks):
        load(i).wait()
        x = held_ref[i * block : (i + 1) * block, :]
        squares = column_squares(x)
        product = gram_tile(x[:, :B], x[:, B:])
        if i == 0:
            n_acc[...] = squares
            c_acc[...] = product
        else:
            n_acc[...] += squares
            c_acc[...] += product
    norms = jnp.sum(n_acc[...], axis=0, keepdims=True)
    o_ref[:B, :] = c_acc[...]
    o_ref[B:, :] = jnp.concatenate(
        [norms[:, :B], norms[:, B:], jnp.zeros((PACK - B - 2, B), F32)], axis=0
    )


def first_gram(matrix):
    rows = matrix.shape[0]
    return pl.pallas_call(
        functools.partial(gram_body, 8),
        in_specs=[HBM],
        out_specs=VM,
        out_shape=jax.ShapeDtypeStruct((PACK, B), F32),
        scratch_shapes=[
            pltpu.VMEM(matrix.shape, F32),
            pltpu.VMEM((B, B), F32),
            pltpu.VMEM((8, 2 * B), F32),
            pltpu.SemaphoreType.DMA((8,)),
        ],
        compiler_params=params(52),
        cost_estimate=cost(rows * B * B * 8, rows * B * 8),
        name="first_gram",
    )(matrix)


def root_body(a_ref, b_ref, c_ref, d_ref, wh_ref, wl_ref, s_ref):
    total = (a_ref[...] + b_ref[...]) + (c_ref[...] + d_ref[...])
    inverse = lax.rsqrt(total[B : B + 8, :])
    first = jnp.broadcast_to(inverse[0:1, :], (B, B)).T
    cosines = total[:B, :] * first * inverse[1:2, :]
    squares = jnp.sum(cosines * cosines)
    k = 0.5 * cosines
    scale = 1.0 + jnp.sum(k * k)
    kt = k.T
    row = lax.broadcasted_iota(jnp.int32, (B, B), 0)
    col = lax.broadcasted_iota(jnp.int32, (B, B), 1)
    eye = (row == col).astype(F32)
    ks, kts = halves(k), halves(kt)
    current = [(eye + split_dot(ks, kts)) / scale, (eye + split_dot(kts, ks)) / scale]
    result = [None, None]
    for step in range(NS_ITERS):
        for side in range(2):
            ys = halves(current[side])
            if step == 0:
                factor = 1.5 * eye - 0.5 * current[side]
                fs = halves(factor)
                result[side] = factor
            else:
                zs = halves(result[side])
                factor = 1.5 * eye - 0.5 * split_dot(zs, ys)
                fs = halves(factor)
                result[side] = split_dot(fs, zs)
            if step < NS_ITERS - 1:
                current[side] = split_dot(ys, fs)
    root = lax.sqrt(jnp.full((1, B), scale, F32))
    q1 = result[0] / root
    q2 = result[1] / root
    q1s, q2s = halves(q1), halves(q2)
    corner = split_dot(ks, q2s)
    lower = -split_dot(kts, q1s)
    for value, rows, cols in ((q1, 0, 0), (corner, 0, B), (lower, B, 0), (q2, B, B)):
        high, low = halves(value)
        wh_ref[rows : rows + B, cols : cols + B] = high
        wl_ref[rows : rows + B, cols : cols + B] = low
    s_ref[...] = jnp.full((8, B), squares, F32)


def roots(parts):
    return pl.pallas_call(
        root_body,
        in_specs=[VM] * 4,
        out_specs=[VM] * 3,
        out_shape=[
            jax.ShapeDtypeStruct((2 * B, 2 * B), BF16),
            jax.ShapeDtypeStruct((2 * B, 2 * B), BF16),
            jax.ShapeDtypeStruct((8, B), F32),
        ],
        compiler_params=params(8),
        cost_estimate=cost(30e6, 1e6),
        name="roots",
    )(*parts)


def mixed(x, wh, wl):
    rows = x.shape[0]
    xh, xl = halves(x)
    both = dot(jnp.concatenate([xh, xl], axis=0), wh)
    return both[:rows] + (both[rows:] + dot(xh, wl))


def update_body(start, sizes, m_ref, wh_ref, wl_ref, *outs):
    wh, wl = wh_ref[...], wl_ref[...]
    at = start
    for n, size in enumerate(sizes):
        value = mixed(m_ref[at : at + size, :], wh, wl)
        outs[2 * n][...] = value[:, :B]
        outs[2 * n + 1][...] = value[:, B:]
        at += size


def update(matrix, w, start, sizes):
    shapes = []
    for size in sizes:
        shapes += [jax.ShapeDtypeStruct((size, B), F32)] * 2
    total = sum(sizes)
    outs = pl.pallas_call(
        functools.partial(update_body, start, tuple(sizes)),
        in_specs=[VM] * 3,
        out_specs=[VM] * len(shapes),
        out_shape=shapes,
        compiler_params=params(12),
        cost_estimate=cost(6 * total * 256 * 256, total * B * 16),
    )(matrix, *w)
    return outs[0::2], outs[1::2]


def partial_body(count, right_only, with_right, *refs):
    lefts = refs[:count]
    rights = refs[count : 2 * count]
    extra = refs[2 * count : 2 * count + right_only]
    o_ref = refs[-1]
    acc = jnp.zeros((B, B), F32)
    lsq = jnp.zeros((8, B), F32)
    rsq = jnp.zeros((8, B), F32)
    for left, right in zip(lefts, rights):
        x, y = left[...], right[...]
        acc = acc + gram_tile(x, y)
        lsq = lsq + column_squares(x)
        if with_right:
            rsq = rsq + column_squares(y)
    for right in extra:
        rsq = rsq + column_squares(right[...])
    tail = jnp.concatenate(
        [
            jnp.sum(lsq, axis=0, keepdims=True),
            jnp.sum(rsq, axis=0, keepdims=True),
            jnp.zeros((PACK - B - 2, B), F32),
        ],
        axis=0,
    )
    for base in refs[2 * count + right_only : -1]:
        acc = acc + base[:B, :]
        tail = tail + base[B:, :]
    o_ref[:B, :] = acc
    o_ref[B:, :] = tail


def partial(lefts, rights, extra, bases, with_right=True):
    total = sum(x.shape[0] for x in lefts)
    operands = [*lefts, *rights, *extra, *bases]
    return pl.pallas_call(
        functools.partial(partial_body, len(lefts), len(extra), with_right),
        in_specs=[VM] * len(operands),
        out_specs=VM,
        out_shape=jax.ShapeDtypeStruct((PACK, B), F32),
        compiler_params=params(12),
        cost_estimate=cost(total * B * B * 8, total * B * 8),
    )(*operands)


def second_body(rows0, aliased, count, *refs):
    xs = refs[:count]
    rs = refs[count : 2 * count]
    wh_ref, wl_ref = refs[2 * count : 2 * count + 2]
    rest = refs[2 * count + 2 + (1 if aliased else 0) :]
    out = rest[0]
    ys = rest[1 : 1 + count]
    held, sem = rest[1 + count :]
    wh, wl = wh_ref[...], wl_ref[...]
    at = 0
    for x, r, y in zip(xs, rs, ys):
        size = x.shape[0]
        value = mixed(jnp.concatenate([x[...], r[...]], axis=1), wh, wl)
        held[at : at + size, :] = value[:, :B]
        y[...] = value[:, B:]
        at += size
    copy = pltpu.make_async_copy(held, out.at[pl.ds(rows0, at), pl.ds(0, B)], sem)
    copy.start()
    copy.wait()


def second(xs, rs, w, out, rows, rows0):
    total = sum(x.shape[0] for x in xs)
    shapes = [jax.ShapeDtypeStruct((rows, 2 * B), F32)] + [
        jax.ShapeDtypeStruct(x.shape, F32) for x in xs
    ]
    operands = [*xs, *rs, *w] + ([out] if out is not None else [])
    specs = [VM] * (2 * len(xs) + 2) + ([HBM] if out is not None else [])
    return pl.pallas_call(
        functools.partial(second_body, rows0, out is not None, len(xs)),
        in_specs=specs,
        out_specs=[HBM] + [VM] * len(xs),
        out_shape=shapes,
        scratch_shapes=[pltpu.VMEM((total, B), F32), pltpu.SemaphoreType.DMA],
        input_output_aliases={} if out is None else {len(operands) - 1: 0},
        compiler_params=params(12),
        cost_estimate=cost(6 * total * 256 * 256, total * B * 20),
    )(*operands)


def place_body(starts, *refs):
    count = len(starts)
    ys = refs[:count]
    out = refs[count + 1]
    sems = refs[count + 2]
    copies = []
    for n, (y, start) in enumerate(zip(ys, starts)):
        copies.append(
            pltpu.make_async_copy(
                y, out.at[pl.ds(start, y.shape[0]), pl.ds(B, B)], sems.at[n]
            )
        )
    for copy in copies:
        copy.start()
    for copy in copies:
        copy.wait()


def place(ys, starts, out):
    return pl.pallas_call(
        functools.partial(place_body, tuple(starts)),
        in_specs=[ANY] * len(ys) + [HBM],
        out_specs=HBM,
        out_shape=jax.ShapeDtypeStruct(out.shape, F32),
        scratch_shapes=[pltpu.SemaphoreType.DMA((len(ys),))],
        input_output_aliases={len(ys): 0},
        compiler_params=params(8),
        cost_estimate=cost(1, sum(y.size for y in ys) * 8),
    )(*ys, out)


def shifted(value, steps):
    count = lax.axis_size("blk")
    return lax.ppermute(value, "blk", [(s, (s + steps) % count) for s in range(count)])


def of_group(value):
    count = lax.axis_size("row")
    parts = [value]
    for mask in range(1, count):
        parts.append(lax.ppermute(value, "row", [(s, s ^ mask) for s in range(count)]))
    return parts


def moved(value, where):
    count = lax.axis_size("blk")
    return lax.ppermute(value, "blk", [(s, where(s)) for s in range(count)])


def of_all_pairs(values):
    count = lax.axis_size("blk")
    inner = 8 if count % 8 == 0 else count
    middle = 4 if count % (4 * inner) == 0 else 1

    def along_inner(steps):
        return lambda s: s // inner * inner + (s + steps) % inner

    def along_middle(steps):
        ring = inner * middle
        return lambda s: s // ring * ring + (s + steps * inner) % ring

    def gathered(tile, moves):
        for part in [moved(tile, where) for where in moves]:
            tile = jnp.maximum(tile, part)
        return tile

    lane = lax.broadcasted_iota(jnp.int32, (8, B), 1)
    at = STEPS * lax.axis_index("blk")
    tile = jnp.zeros((8, B), F32)
    for step, value in enumerate(values):
        tile = jnp.where(lane == at + step, value, tile)
    if middle > 1:
        tile = gathered(tile, [along_middle(n) for n in range(1, middle)])
    outer = count // (inner * middle)
    if outer > 1:
        tile = gathered(
            tile,
            [
                lambda s, n=n: (s + n * inner * middle) % count
                for n in range(1, outer)
            ],
        )
    reach = 1
    for width in (3, 1, 1):
        if reach >= inner:
            break
        if width == 3:
            tile = gathered(tile, [along_inner(-n) for n in range(1, min(4, inner))])
            reach = min(4, inner)
        else:
            step = min(3, inner - reach)
            tile = gathered(tile, [along_inner(-step)])
            reach += step
    return tile[0, : STEPS * count].reshape(count, STEPS)


def steps(matrix):
    rows = matrix.shape[0]
    unit = rows // UNITS
    front = [n * unit for n in FRONT]
    back = [n * unit for n in BACK]
    front_rows = sum(front)

    wh, wl, squares0 = roots(of_group(first_gram(matrix)))
    w = (wh, wl)

    xf, rf = update(matrix, w, 0, front[:1])
    xb, rb = update(matrix, w, front_rows, back)
    more_x, more_r = update(matrix, w, front[0], front[1:])
    xf, rf = [*xf, *more_x], [*rf, *more_r]

    got = [shifted(x, 1) for x in xf]
    behind = [shifted(r, -1) for r in rb]
    helped = shifted(partial(xb, behind, [], [], False), 1)
    got_back = [shifted(x, 1) for x in xb]

    cut = len(got) - 1
    sums = partial(got[:cut], rf[:cut], rb, [])
    sums = partial(got[cut:], rf[cut:], [], [sums, helped])
    wh, wl, squares1 = roots(of_group(sums))
    w = (wh, wl)

    out, *ys = second(got[:1], rf[:1], w, None, rows, 0)
    out, *more_y = second(got[1:], rf[1:], w, out, rows, front[0])
    out, *back_y = second(got_back, rb, w, out, rows, front_rows)
    ys = [*ys, *more_y, *back_y]
    arrived = [shifted(y, 1) for y in ys]

    totals = jnp.sum(of_all_pairs([squares0, squares1]), axis=0)
    off_measure = totals / float(lax.axis_size("blk"))
    places, at = [], 0
    for y in ys:
        places.append(at)
        at += y.shape[0]
    out = place(arrived, places, out)
    return out, off_measure


def solution(mesh):
    return jax.shard_map(
        steps,
        mesh=mesh,
        in_specs=(P("row", "blk"),),
        out_specs=(P("row", "blk"), P()),
        check_vma=False,
    )
```

```python
import functools

import jax
import jax.numpy as jnp
from jax import lax
from jax.experimental import pallas as pl
from jax.experimental.pallas import tpu as pltpu
from jax.sharding import PartitionSpec as P


STEPS = 2
NS_ITERS = 4
B = 128
PACK = 136
UNITS = 32
FRONT = (4, 4, 4, 4, 4, 2)
BACK = (5, 3, 2)

VM = pl.BlockSpec(memory_space=pltpu.VMEM)
ANY = pl.BlockSpec(memory_space=pl.ANY)
HBM = pl.BlockSpec(memory_space=pltpu.HBM)
F32 = jnp.float32
BF16 = jnp.bfloat16


def params(mib=24):
    return pltpu.CompilerParams(vmem_limit_bytes=mib * 1024 * 1024)


def cost(flops, moved):
    return pl.CostEstimate(flops=int(flops), bytes_accessed=int(moved), transcendentals=0)


def halves(x):
    high = x.astype(BF16)
    low = (x - high.astype(F32)).astype(BF16)
    return high, low


def dot(a, b):
    return jnp.dot(a, b, preferred_element_type=F32)


def dot_rows(a, b):
    return lax.dot_general(a, b, (((0,), (0,)), ((), ())), preferred_element_type=F32)


def split_dot(a, b):
    ah, al = a
    bh, bl = b
    return dot(ah, bh) + (dot(ah, bl) + dot(al, bh))


def gram_tile(left, right):
    lh, ll = halves(left)
    rh, rl = halves(right)
    full = dot_rows(jnp.concatenate([lh, ll], 1), jnp.concatenate([rh, rl], 1))
    return (full[:B, :B] + full[B:, B:]) + (full[:B, B:] + full[B:, :B])


def column_squares(x):
    return jnp.sum((x * x).reshape(x.shape[0] // 8, 8, x.shape[1]), axis=0)


def gram_body(blocks, m_ref, o_ref, held_ref, c_acc, n_acc, sems):
    block = m_ref.shape[0] // blocks

    def load(i):
        rows = pl.ds(i * block, block)
        return pltpu.make_async_copy(m_ref.at[rows, :], held_ref.at[rows, :], sems.at[i])

    for i in range(blocks):
        load(i).start()
    for i in range(blocks):
        load(i).wait()
        x = held_ref[i * block : (i + 1) * block, :]
        squares = column_squares(x)
        product = gram_tile(x[:, :B], x[:, B:])
        if i == 0:
            n_acc[...] = squares
            c_acc[...] = product
        else:
            n_acc[...] += squares
            c_acc[...] += product
    norms = jnp.sum(n_acc[...], axis=0, keepdims=True)
    o_ref[:B, :] = c_acc[...]
    o_ref[B:, :] = jnp.concatenate(
        [norms[:, :B], norms[:, B:], jnp.zeros((PACK - B - 2, B), F32)], axis=0
    )


def first_gram(matrix):
    rows = matrix.shape[0]
    return pl.pallas_call(
        functools.partial(gram_body, 8),
        in_specs=[HBM],
        out_specs=VM,
        out_shape=jax.ShapeDtypeStruct((PACK, B), F32),
        scratch_shapes=[
            pltpu.VMEM(matrix.shape, F32),
            pltpu.VMEM((B, B), F32),
            pltpu.VMEM((8, 2 * B), F32),
            pltpu.SemaphoreType.DMA((8,)),
        ],
        compiler_params=params(52),
        cost_estimate=cost(rows * B * B * 8, rows * B * 8),
        name="first_gram",
    )(matrix)


def root_body(a_ref, b_ref, wh_ref, wl_ref, s_ref):
    total = a_ref[...] + b_ref[...]
    inverse = lax.rsqrt(total[B : B + 8, :])
    first = jnp.broadcast_to(inverse[0:1, :], (B, B)).T
    cosines = total[:B, :] * first * inverse[1:2, :]
    squares = jnp.sum(cosines * cosines)
    k = 0.5 * cosines
    scale = 1.0 + jnp.sum(k * k)
    kt = k.T
    row = lax.broadcasted_iota(jnp.int32, (B, B), 0)
    col = lax.broadcasted_iota(jnp.int32, (B, B), 1)
    eye = (row == col).astype(F32)
    ks, kts = halves(k), halves(kt)
    current = [(eye + split_dot(ks, kts)) / scale, (eye + split_dot(kts, ks)) / scale]
    result = [None, None]
    for step in range(NS_ITERS):
        for side in range(2):
            ys = halves(current[side])
            if step == 0:
                factor = 1.5 * eye - 0.5 * current[side]
                fs = halves(factor)
                result[side] = factor
            else:
                zs = halves(result[side])
                factor = 1.5 * eye - 0.5 * split_dot(zs, ys)
                fs = halves(factor)
                result[side] = split_dot(fs, zs)
            if step < NS_ITERS - 1:
                current[side] = split_dot(ys, fs)
    root = lax.sqrt(jnp.full((1, B), scale, F32))
    q1 = result[0] / root
    q2 = result[1] / root
    q1s, q2s = halves(q1), halves(q2)
    corner = split_dot(ks, q2s)
    lower = -split_dot(kts, q1s)
    for value, rows, cols in ((q1, 0, 0), (corner, 0, B), (lower, B, 0), (q2, B, B)):
        high, low = halves(value)
        wh_ref[rows : rows + B, cols : cols + B] = high
        wl_ref[rows : rows + B, cols : cols + B] = low
    s_ref[...] = jnp.full((8, B), squares, F32)


def roots(parts):
    return pl.pallas_call(
        root_body,
        in_specs=[VM] * 2,
        out_specs=[VM] * 3,
        out_shape=[
            jax.ShapeDtypeStruct((2 * B, 2 * B), BF16),
            jax.ShapeDtypeStruct((2 * B, 2 * B), BF16),
            jax.ShapeDtypeStruct((8, B), F32),
        ],
        compiler_params=params(8),
        cost_estimate=cost(30e6, 1e6),
        name="roots",
    )(*parts)


def mixed(x, wh, wl):
    rows = x.shape[0]
    xh, xl = halves(x)
    both = dot(jnp.concatenate([xh, xl], axis=0), wh)
    return both[:rows] + (both[rows:] + dot(xh, wl))


def update_body(start, sizes, m_ref, wh_ref, wl_ref, *outs):
    wh, wl = wh_ref[...], wl_ref[...]
    at = start
    for n, size in enumerate(sizes):
        value = mixed(m_ref[at : at + size, :], wh, wl)
        outs[2 * n][...] = value[:, :B]
        outs[2 * n + 1][...] = value[:, B:]
        at += size


def update(matrix, w, start, sizes):
    shapes = []
    for size in sizes:
        shapes += [jax.ShapeDtypeStruct((size, B), F32)] * 2
    total = sum(sizes)
    outs = pl.pallas_call(
        functools.partial(update_body, start, tuple(sizes)),
        in_specs=[VM] * 3,
        out_specs=[VM] * len(shapes),
        out_shape=shapes,
        compiler_params=params(12),
        cost_estimate=cost(6 * total * 256 * 256, total * B * 16),
    )(matrix, *w)
    return outs[0::2], outs[1::2]


def partial_body(count, right_only, with_right, *refs):
    lefts = refs[:count]
    rights = refs[count : 2 * count]
    extra = refs[2 * count : 2 * count + right_only]
    o_ref = refs[-1]
    acc = jnp.zeros((B, B), F32)
    lsq = jnp.zeros((8, B), F32)
    rsq = jnp.zeros((8, B), F32)
    for left, right in zip(lefts, rights):
        x, y = left[...], right[...]
        acc = acc + gram_tile(x, y)
        lsq = lsq + column_squares(x)
        if with_right:
            rsq = rsq + column_squares(y)
    for right in extra:
        rsq = rsq + column_squares(right[...])
    tail = jnp.concatenate(
        [
            jnp.sum(lsq, axis=0, keepdims=True),
            jnp.sum(rsq, axis=0, keepdims=True),
            jnp.zeros((PACK - B - 2, B), F32),
        ],
        axis=0,
    )
    for base in refs[2 * count + right_only : -1]:
        acc = acc + base[:B, :]
        tail = tail + base[B:, :]
    o_ref[:B, :] = acc
    o_ref[B:, :] = tail


def partial(lefts, rights, extra, bases, with_right=True):
    total = sum(x.shape[0] for x in lefts)
    operands = [*lefts, *rights, *extra, *bases]
    return pl.pallas_call(
        functools.partial(partial_body, len(lefts), len(extra), with_right),
        in_specs=[VM] * len(operands),
        out_specs=VM,
        out_shape=jax.ShapeDtypeStruct((PACK, B), F32),
        compiler_params=params(12),
        cost_estimate=cost(total * B * B * 8, total * B * 8),
    )(*operands)


def second_body(rows0, aliased, count, *refs):
    xs = refs[:count]
    rs = refs[count : 2 * count]
    wh_ref, wl_ref = refs[2 * count : 2 * count + 2]
    rest = refs[2 * count + 2 + (1 if aliased else 0) :]
    out = rest[0]
    ys = rest[1 : 1 + count]
    held, sem = rest[1 + count :]
    wh, wl = wh_ref[...], wl_ref[...]
    at = 0
    for x, r, y in zip(xs, rs, ys):
        size = x.shape[0]
        value = mixed(jnp.concatenate([x[...], r[...]], axis=1), wh, wl)
        held[at : at + size, :] = value[:, :B]
        y[...] = value[:, B:]
        at += size
    copy = pltpu.make_async_copy(held, out.at[pl.ds(rows0, at), pl.ds(0, B)], sem)
    copy.start()
    copy.wait()


def second(xs, rs, w, out, rows, rows0):
    total = sum(x.shape[0] for x in xs)
    shapes = [jax.ShapeDtypeStruct((rows, 2 * B), F32)] + [
        jax.ShapeDtypeStruct(x.shape, F32) for x in xs
    ]
    operands = [*xs, *rs, *w] + ([out] if out is not None else [])
    specs = [VM] * (2 * len(xs) + 2) + ([HBM] if out is not None else [])
    return pl.pallas_call(
        functools.partial(second_body, rows0, out is not None, len(xs)),
        in_specs=specs,
        out_specs=[HBM] + [VM] * len(xs),
        out_shape=shapes,
        scratch_shapes=[pltpu.VMEM((total, B), F32), pltpu.SemaphoreType.DMA],
        input_output_aliases={} if out is None else {len(operands) - 1: 0},
        compiler_params=params(12),
        cost_estimate=cost(6 * total * 256 * 256, total * B * 20),
    )(*operands)


def place_body(starts, *refs):
    count = len(starts)
    ys = refs[:count]
    out = refs[count + 1]
    sems = refs[count + 2]
    copies = []
    for n, (y, start) in enumerate(zip(ys, starts)):
        copies.append(
            pltpu.make_async_copy(
                y, out.at[pl.ds(start, y.shape[0]), pl.ds(B, B)], sems.at[n]
            )
        )
    for copy in copies:
        copy.start()
    for copy in copies:
        copy.wait()


def place(ys, starts, out):
    return pl.pallas_call(
        functools.partial(place_body, tuple(starts)),
        in_specs=[VM] * len(ys) + [HBM],
        out_specs=HBM,
        out_shape=jax.ShapeDtypeStruct(out.shape, F32),
        scratch_shapes=[pltpu.SemaphoreType.DMA((len(ys),))],
        input_output_aliases={len(ys): 0},
        compiler_params=params(8),
        cost_estimate=cost(1, sum(y.size for y in ys) * 8),
    )(*ys, out)


def shifted(value, steps):
    count = lax.axis_size("blk")
    return lax.ppermute(value, "blk", [(s, (s + steps) % count) for s in range(count)])


def of_group(value):
    count = lax.axis_size("row")

    def from_other(part, mask):
        return lax.ppermute(part, "row", [(s, s ^ mask) for s in range(count)])

    mask = 1
    while 2 * mask < count:
        value = value + from_other(value, mask)
        mask *= 2
    return value, from_other(value, mask)


def moved(value, where):
    count = lax.axis_size("blk")
    return lax.ppermute(value, "blk", [(s, where(s)) for s in range(count)])


def of_all_pairs(values):
    count = lax.axis_size("blk")
    inner = 8 if count % 8 == 0 else count
    middle = 4 if count % (4 * inner) == 0 else 1

    def along_inner(steps):
        return lambda s: s // inner * inner + (s + steps) % inner

    def along_middle(steps):
        ring = inner * middle
        return lambda s: s // ring * ring + (s + steps * inner) % ring

    def gathered(tile, moves):
        for part in [moved(tile, where) for where in moves]:
            tile = jnp.maximum(tile, part)
        return tile

    lane = lax.broadcasted_iota(jnp.int32, (8, B), 1)
    at = STEPS * lax.axis_index("blk")
    tile = jnp.zeros((8, B), F32)
    for step, value in enumerate(values):
        tile = jnp.where(lane == at + step, value, tile)
    reach = min(4, inner)
    if inner > 1:
        tile = gathered(tile, [along_inner(-n) for n in range(1, reach)])
    while reach < inner:
        step = min(3, inner - reach)
        tile = gathered(tile, [along_inner(-step)])
        reach += step
    for _ in range(1, middle):
        tile = gathered(tile, [along_middle(-1)])
    outer = count // (inner * middle)
    for n in range(1, outer):
        tile = gathered(tile, [lambda s, n=n: (s + n * inner * middle) % count])
    return tile[0, : STEPS * count].reshape(count, STEPS)


def steps(matrix):
    rows = matrix.shape[0]
    unit = rows // UNITS
    front = [n * unit for n in FRONT]
    back = [n * unit for n in BACK]
    front_rows = sum(front)

    wh, wl, squares0 = roots(of_group(first_gram(matrix)))
    w = (wh, wl)

    xf, rf = update(matrix, w, 0, front[:1])
    more_x, more_r = update(matrix, w, front[0], front[1:])
    xb, rb = update(matrix, w, front_rows, back)
    xf, rf = [*xf, *more_x], [*rf, *more_r]

    got = [shifted(x, 1) for x in xf]
    behind = [shifted(r, -1) for r in rb]
    helped = shifted(partial(xb, behind, [], [], False), 1)
    got_back = [shifted(x, 1) for x in xb]

    cut = len(got) - 1
    sums = partial(got[:cut], rf[:cut], rb, [])
    sums = partial(got[cut:], rf[cut:], [], [sums, helped])
    wh, wl, squares1 = roots(of_group(sums))
    w = (wh, wl)

    out, *ys = second(got[:1], rf[:1], w, None, rows, 0)
    out, *more_y = second(got[1:], rf[1:], w, out, rows, front[0])
    out, *back_y = second(got_back, rb, w, out, rows, front_rows)
    ys = [*ys, *more_y, *back_y]
    arrived = [shifted(y, 1) for y in ys]

    totals = jnp.sum(of_all_pairs([squares0, squares1]), axis=0)
    off_measure = totals / float(lax.axis_size("blk"))
    places, at = [], 0
    for y in ys:
        places.append(at)
        at += y.shape[0]
    for lo, hi in ((0, 6), (6, 8), (8, 9)):
        out = place(arrived[lo:hi], places[lo:hi], out)
    return out, off_measure


def solution(mesh):
    return jax.shard_map(
        steps,
        mesh=mesh,
        in_specs=(P("row", "blk"),),
        out_specs=(P("row", "blk"), P()),
        check_vma=False,
    )
```

```python
import functools

import jax
import jax.numpy as jnp
from jax import lax
from jax.experimental import pallas as pl
from jax.experimental.pallas import tpu as pltpu
from jax.sharding import PartitionSpec as P


STEPS = 2
NS_ITERS = 4
B = 128
PACK = 136
UNITS = 32
FRONT = (4, 4, 4, 4, 4, 2)
BACK = (5, 3, 2)

VM = pl.BlockSpec(memory_space=pltpu.VMEM)
ANY = pl.BlockSpec(memory_space=pl.ANY)
HBM = pl.BlockSpec(memory_space=pltpu.HBM)
F32 = jnp.float32
BF16 = jnp.bfloat16


def params(mib=24):
    return pltpu.CompilerParams(vmem_limit_bytes=mib * 1024 * 1024)


def cost(flops, moved):
    return pl.CostEstimate(flops=int(flops), bytes_accessed=int(moved), transcendentals=0)


def halves(x):
    high = x.astype(BF16)
    low = (x - high.astype(F32)).astype(BF16)
    return high, low


def dot(a, b):
    return jnp.dot(a, b, preferred_element_type=F32)


def dot_rows(a, b):
    return lax.dot_general(a, b, (((0,), (0,)), ((), ())), preferred_element_type=F32)


def split_dot(a, b):
    ah, al = a
    bh, bl = b
    return dot(ah, bh) + (dot(ah, bl) + dot(al, bh))


def gram_tile(left, right):
    lh, ll = halves(left)
    rh, rl = halves(right)
    full = dot_rows(jnp.concatenate([lh, ll], 1), jnp.concatenate([rh, rl], 1))
    return (full[:B, :B] + full[B:, B:]) + (full[:B, B:] + full[B:, :B])


def column_squares(x):
    return jnp.sum((x * x).reshape(x.shape[0] // 8, 8, x.shape[1]), axis=0)


def gram_body(blocks, m_ref, o_ref, held_ref, c_acc, n_acc, sems):
    block = m_ref.shape[0] // blocks

    def load(i):
        rows = pl.ds(i * block, block)
        return pltpu.make_async_copy(m_ref.at[rows, :], held_ref.at[rows, :], sems.at[i])

    for i in range(blocks):
        load(i).start()
    for i in range(blocks):
        load(i).wait()
        x = held_ref[i * block : (i + 1) * block, :]
        squares = column_squares(x)
        product = gram_tile(x[:, :B], x[:, B:])
        if i == 0:
            n_acc[...] = squares
            c_acc[...] = product
        else:
            n_acc[...] += squares
            c_acc[...] += product
    norms = jnp.sum(n_acc[...], axis=0, keepdims=True)
    o_ref[:B, :] = c_acc[...]
    o_ref[B:, :] = jnp.concatenate(
        [norms[:, :B], norms[:, B:], jnp.zeros((PACK - B - 2, B), F32)], axis=0
    )


def first_gram(matrix):
    rows = matrix.shape[0]
    return pl.pallas_call(
        functools.partial(gram_body, 8),
        in_specs=[HBM],
        out_specs=VM,
        out_shape=jax.ShapeDtypeStruct((PACK, B), F32),
        scratch_shapes=[
            pltpu.VMEM(matrix.shape, F32),
            pltpu.VMEM((B, B), F32),
            pltpu.VMEM((8, 2 * B), F32),
            pltpu.SemaphoreType.DMA((8,)),
        ],
        compiler_params=params(52),
        cost_estimate=cost(rows * B * B * 8, rows * B * 8),
        name="first_gram",
    )(matrix)


def root_body(slot, a_ref, b_ref, wh_ref, wl_ref, s_ref):
    total = a_ref[...] + b_ref[...]
    inverse = lax.rsqrt(total[B : B + 8, :])
    first = jnp.broadcast_to(inverse[0:1, :], (B, B)).T
    cosines = total[:B, :] * first * inverse[1:2, :]
    squares = jnp.sum(cosines * cosines)
    k = 0.5 * cosines
    scale = 1.0 + jnp.sum(k * k)
    kt = k.T
    row = lax.broadcasted_iota(jnp.int32, (B, B), 0)
    col = lax.broadcasted_iota(jnp.int32, (B, B), 1)
    eye = (row == col).astype(F32)
    ks, kts = halves(k), halves(kt)
    current = [(eye + split_dot(ks, kts)) / scale, (eye + split_dot(kts, ks)) / scale]
    result = [None, None]
    for step in range(NS_ITERS):
        for side in range(2):
            ys = halves(current[side])
            if step == 0:
                factor = 1.5 * eye - 0.5 * current[side]
                fs = halves(factor)
                result[side] = factor
            else:
                zs = halves(result[side])
                factor = 1.5 * eye - 0.5 * split_dot(zs, ys)
                fs = halves(factor)
                result[side] = split_dot(fs, zs)
            if step < NS_ITERS - 1:
                current[side] = split_dot(ys, fs)
    root = lax.sqrt(jnp.full((1, B), scale, F32))
    q1 = result[0] / root
    q2 = result[1] / root
    q1s, q2s = halves(q1), halves(q2)
    corner = split_dot(ks, q2s)
    lower = -split_dot(kts, q1s)
    for value, rows, cols in ((q1, 0, 0), (corner, 0, B), (lower, B, 0), (q2, B, B)):
        high, low = halves(value)
        wh_ref[rows : rows + B, cols : cols + B] = high
        wl_ref[rows : rows + B, cols : cols + B] = low
    lane = lax.broadcasted_iota(jnp.int32, (8, B), 1)
    own = STEPS * lax.axis_index("blk") + slot
    s_ref[...] = jnp.where(lane == own, squares, 0.0)


def roots(parts, slot):
    return pl.pallas_call(
        functools.partial(root_body, slot),
        in_specs=[VM] * 2,
        out_specs=[VM] * 3,
        out_shape=[
            jax.ShapeDtypeStruct((2 * B, 2 * B), BF16),
            jax.ShapeDtypeStruct((2 * B, 2 * B), BF16),
            jax.ShapeDtypeStruct((8, B), F32),
        ],
        compiler_params=params(8),
        cost_estimate=cost(30e6, 1e6),
        name="roots",
    )(*parts)


def mixed(x, wh, wl):
    rows = x.shape[0]
    xh, xl = halves(x)
    both = dot(jnp.concatenate([xh, xl], axis=0), wh)
    return both[:rows] + (both[rows:] + dot(xh, wl))


def update_body(start, sizes, m_ref, wh_ref, wl_ref, *outs):
    wh, wl = wh_ref[...], wl_ref[...]
    at = start
    for n, size in enumerate(sizes):
        value = mixed(m_ref[at : at + size, :], wh, wl)
        outs[2 * n][...] = value[:, :B]
        outs[2 * n + 1][...] = value[:, B:]
        at += size


def update(matrix, w, start, sizes):
    shapes = []
    for size in sizes:
        shapes += [jax.ShapeDtypeStruct((size, B), F32)] * 2
    total = sum(sizes)
    outs = pl.pallas_call(
        functools.partial(update_body, start, tuple(sizes)),
        in_specs=[VM] * 3,
        out_specs=[VM] * len(shapes),
        out_shape=shapes,
        compiler_params=params(12),
        cost_estimate=cost(6 * total * 256 * 256, total * B * 16),
    )(matrix, *w)
    return outs[0::2], outs[1::2]


def partial_body(count, right_only, with_right, *refs):
    lefts = refs[:count]
    rights = refs[count : 2 * count]
    extra = refs[2 * count : 2 * count + right_only]
    o_ref = refs[-1]
    acc = jnp.zeros((B, B), F32)
    lsq = jnp.zeros((8, B), F32)
    rsq = jnp.zeros((8, B), F32)
    for left, right in zip(lefts, rights):
        x, y = left[...], right[...]
        acc = acc + gram_tile(x, y)
        lsq = lsq + column_squares(x)
        if with_right:
            rsq = rsq + column_squares(y)
    for right in extra:
        rsq = rsq + column_squares(right[...])
    tail = jnp.concatenate(
        [
            jnp.sum(lsq, axis=0, keepdims=True),
            jnp.sum(rsq, axis=0, keepdims=True),
            jnp.zeros((PACK - B - 2, B), F32),
        ],
        axis=0,
    )
    for base in refs[2 * count + right_only : -1]:
        acc = acc + base[:B, :]
        tail = tail + base[B:, :]
    o_ref[:B, :] = acc
    o_ref[B:, :] = tail


def partial(lefts, rights, extra, bases, with_right=True):
    total = sum(x.shape[0] for x in lefts)
    operands = [*lefts, *rights, *extra, *bases]
    return pl.pallas_call(
        functools.partial(partial_body, len(lefts), len(extra), with_right),
        in_specs=[VM] * len(operands),
        out_specs=VM,
        out_shape=jax.ShapeDtypeStruct((PACK, B), F32),
        compiler_params=params(12),
        cost_estimate=cost(total * B * B * 8, total * B * 8),
    )(*operands)


def second_body(rows0, aliased, count, *refs):
    xs = refs[:count]
    rs = refs[count : 2 * count]
    wh_ref, wl_ref = refs[2 * count : 2 * count + 2]
    rest = refs[2 * count + 2 + (1 if aliased else 0) :]
    out = rest[0]
    ys = rest[1 : 1 + count]
    held, sem = rest[1 + count :]
    wh, wl = wh_ref[...], wl_ref[...]
    at = 0
    for x, r, y in zip(xs, rs, ys):
        size = x.shape[0]
        value = mixed(jnp.concatenate([x[...], r[...]], axis=1), wh, wl)
        held[at : at + size, :] = value[:, :B]
        y[...] = value[:, B:]
        at += size
    copy = pltpu.make_async_copy(held, out.at[pl.ds(rows0, at), pl.ds(0, B)], sem)
    copy.start()
    copy.wait()


def second(xs, rs, w, out, rows, rows0):
    total = sum(x.shape[0] for x in xs)
    shapes = [jax.ShapeDtypeStruct((rows, 2 * B), F32)] + [
        jax.ShapeDtypeStruct(x.shape, F32) for x in xs
    ]
    operands = [*xs, *rs, *w] + ([out] if out is not None else [])
    specs = [VM] * (2 * len(xs) + 2) + ([HBM] if out is not None else [])
    return pl.pallas_call(
        functools.partial(second_body, rows0, out is not None, len(xs)),
        in_specs=specs,
        out_specs=[HBM] + [VM] * len(xs),
        out_shape=shapes,
        scratch_shapes=[pltpu.VMEM((total, B), F32), pltpu.SemaphoreType.DMA],
        input_output_aliases={} if out is None else {len(operands) - 1: 0},
        compiler_params=params(12),
        cost_estimate=cost(6 * total * 256 * 256, total * B * 20),
    )(*operands)


def place_body(starts, *refs):
    count = len(starts)
    ys = refs[:count]
    out = refs[count + 1]
    sems = refs[count + 2]
    copies = []
    for n, (y, start) in enumerate(zip(ys, starts)):
        copies.append(
            pltpu.make_async_copy(
                y, out.at[pl.ds(start, y.shape[0]), pl.ds(B, B)], sems.at[n]
            )
        )
    for copy in copies:
        copy.start()
    for copy in copies:
        copy.wait()


def place(ys, starts, out):
    return pl.pallas_call(
        functools.partial(place_body, tuple(starts)),
        in_specs=[VM] * len(ys) + [HBM],
        out_specs=HBM,
        out_shape=jax.ShapeDtypeStruct(out.shape, F32),
        scratch_shapes=[pltpu.SemaphoreType.DMA((len(ys),))],
        input_output_aliases={len(ys): 0},
        compiler_params=params(8),
        cost_estimate=cost(1, sum(y.size for y in ys) * 8),
    )(*ys, out)


def shifted(value, steps):
    count = lax.axis_size("blk")
    return lax.ppermute(value, "blk", [(s, (s + steps) % count) for s in range(count)])


def of_group(value):
    count = lax.axis_size("row")

    def from_other(part, mask):
        return lax.ppermute(part, "row", [(s, s ^ mask) for s in range(count)])

    mask = 1
    while 2 * mask < count:
        value = value + from_other(value, mask)
        mask *= 2
    return value, from_other(value, mask)


def moved(value, where):
    count = lax.axis_size("blk")
    return lax.ppermute(value, "blk", [(s, where(s)) for s in range(count)])


def of_all_pairs(tile):
    count = lax.axis_size("blk")
    inner = 8 if count % 8 == 0 else count
    middle = 4 if count % (4 * inner) == 0 else 1
    outer = count // (inner * middle)

    def along_inner(steps):
        return lambda s: s // inner * inner + (s + steps) % inner

    def along_middle(steps):
        ring = inner * middle
        return lambda s: s // ring * ring + (s + steps * inner) % ring

    reach = min(4, inner)
    rounds = [[along_inner(-n) for n in range(1, reach)]]
    while reach < inner:
        step = min(3, inner - reach)
        rounds.append([along_inner(-step)])
        reach += step
    for _ in range(1, middle):
        rounds.append([along_middle(-1)])
    for n in range(1, outer):
        rounds.append([lambda s, n=n: (s + n * inner * middle) % count])
    for moves in rounds:
        for part in [moved(tile, where) for where in moves]:
            tile = jnp.maximum(tile, part)
    return tile


def mean_body(count, t_ref, o_ref):
    lane = lax.broadcasted_iota(jnp.int32, (1, B), 1)
    line = t_ref[0:1, :]
    for step in range(STEPS):
        own = (lane % STEPS == step) & (lane < STEPS * count)
        o_ref[step] = jnp.sum(jnp.where(own, line, 0.0)) / float(count)


def mean_over_pairs(tile):
    return pl.pallas_call(
        functools.partial(mean_body, lax.axis_size("blk")),
        in_specs=[VM],
        out_specs=pl.BlockSpec(memory_space=pltpu.SMEM),
        out_shape=jax.ShapeDtypeStruct((STEPS,), F32),
        compiler_params=params(4),
        cost_estimate=cost(1000, 1000),
        name="mean_over_pairs",
    )(tile)


def steps(matrix):
    rows = matrix.shape[0]
    unit = rows // UNITS
    front = [n * unit for n in FRONT]
    back = [n * unit for n in BACK]
    front_rows = sum(front)

    wh, wl, squares0 = roots(of_group(first_gram(matrix)), 0)
    w = (wh, wl)

    xf, rf = update(matrix, w, 0, front[:1])
    more_x, more_r = update(matrix, w, front[0], front[1:])
    xb, rb = update(matrix, w, front_rows, back)
    xf, rf = [*xf, *more_x], [*rf, *more_r]

    got = [shifted(x, 1) for x in xf]
    behind = [shifted(r, -1) for r in rb]
    helped = shifted(partial(xb, behind, [], [], False), 1)
    got_back = [shifted(x, 1) for x in xb]

    cut = len(got) - 1
    sums = partial(got[:cut], rf[:cut], rb, [])
    sums = partial(got[cut:], rf[cut:], [], [sums, helped])
    wh, wl, squares1 = roots(of_group(sums), 1)
    w = (wh, wl)

    out, *ys = second(got[:1], rf[:1], w, None, rows, 0)
    out, *more_y = second(got[1:], rf[1:], w, out, rows, front[0])
    out, *back_y = second(got_back, rb, w, out, rows, front_rows)
    ys = [*ys, *more_y, *back_y]
    arrived = [shifted(y, 1) for y in ys]

    off_measure = mean_over_pairs(of_all_pairs(jnp.maximum(squares0, squares1)))
    places, at = [], 0
    for y in ys:
        places.append(at)
        at += y.shape[0]
    for lo, hi in ((0, 6), (6, 8), (8, 9)):
        out = place(arrived[lo:hi], places[lo:hi], out)
    return out, off_measure


def solution(mesh):
    return jax.shard_map(
        steps,
        mesh=mesh,
        in_specs=(P("row", "blk"),),
        out_specs=(P("row", "blk"), P()),
        check_vma=False,
    )
```

```python
import functools

import jax
import jax.numpy as jnp
from jax import lax
from jax.experimental import pallas as pl
from jax.experimental.pallas import tpu as pltpu
from jax.sharding import PartitionSpec as P


STEPS = 2
NS_ITERS = 4
B = 128
PACK = 136
UNITS = 32
FRONT = (4, 8, 8)
BACK = (8, 4)
RELAYED = 1

VM = pl.BlockSpec(memory_space=pltpu.VMEM)
ANY = pl.BlockSpec(memory_space=pl.ANY)
HBM = pl.BlockSpec(memory_space=pltpu.HBM)
F32 = jnp.float32
BF16 = jnp.bfloat16


def params(mib=24):
    return pltpu.CompilerParams(vmem_limit_bytes=mib * 1024 * 1024)


def cost(flops, moved):
    return pl.CostEstimate(flops=int(flops), bytes_accessed=int(moved), transcendentals=0)


def halves(x):
    high = x.astype(BF16)
    low = (x - high.astype(F32)).astype(BF16)
    return high, low


def dot(a, b):
    return jnp.dot(a, b, preferred_element_type=F32)


def dot_rows(a, b):
    return lax.dot_general(a, b, (((0,), (0,)), ((), ())), preferred_element_type=F32)


def split_dot(a, b):
    ah, al = a
    bh, bl = b
    return dot(ah, bh) + (dot(ah, bl) + dot(al, bh))


def gram_tile(left, right):
    lh, ll = halves(left)
    rh, rl = halves(right)
    full = dot_rows(jnp.concatenate([lh, ll], 1), jnp.concatenate([rh, rl], 1))
    return (full[:B, :B] + full[B:, B:]) + (full[:B, B:] + full[B:, :B])


def column_squares(x):
    return jnp.sum((x * x).reshape(x.shape[0] // 8, 8, x.shape[1]), axis=0)


def gram_body(blocks, m_ref, o_ref, held_ref, c_acc, n_acc, sems):
    block = m_ref.shape[0] // blocks

    def load(i):
        rows = pl.ds(i * block, block)
        return pltpu.make_async_copy(m_ref.at[rows, :], held_ref.at[rows, :], sems.at[i])

    for i in range(blocks):
        load(i).start()
    for i in range(blocks):
        load(i).wait()
        x = held_ref[i * block : (i + 1) * block, :]
        squares = column_squares(x)
        product = gram_tile(x[:, :B], x[:, B:])
        if i == 0:
            n_acc[...] = squares
            c_acc[...] = product
        else:
            n_acc[...] += squares
            c_acc[...] += product
    norms = jnp.sum(n_acc[...], axis=0, keepdims=True)
    o_ref[:B, :] = c_acc[...]
    o_ref[B:, :] = jnp.concatenate(
        [norms[:, :B], norms[:, B:], jnp.zeros((PACK - B - 2, B), F32)], axis=0
    )


def first_gram(matrix):
    rows = matrix.shape[0]
    return pl.pallas_call(
        functools.partial(gram_body, 8),
        in_specs=[HBM],
        out_specs=VM,
        out_shape=jax.ShapeDtypeStruct((PACK, B), F32),
        scratch_shapes=[
            pltpu.VMEM(matrix.shape, F32),
            pltpu.VMEM((B, B), F32),
            pltpu.VMEM((8, 2 * B), F32),
            pltpu.SemaphoreType.DMA((8,)),
        ],
        compiler_params=params(52),
        cost_estimate=cost(rows * B * B * 8, rows * B * 8),
        name="first_gram",
    )(matrix)


def root_body(slot, a_ref, b_ref, wh_ref, wl_ref, s_ref):
    total = a_ref[...] + b_ref[...]
    inverse = lax.rsqrt(total[B : B + 8, :])
    first = jnp.broadcast_to(inverse[0:1, :], (B, B)).T
    cosines = total[:B, :] * first * inverse[1:2, :]
    squares = jnp.sum(cosines * cosines)
    k = 0.5 * cosines
    scale = 1.0 + jnp.sum(k * k)
    kt = k.T
    row = lax.broadcasted_iota(jnp.int32, (B, B), 0)
    col = lax.broadcasted_iota(jnp.int32, (B, B), 1)
    eye = (row == col).astype(F32)
    ks, kts = halves(k), halves(kt)
    current = [(eye + split_dot(ks, kts)) / scale, (eye + split_dot(kts, ks)) / scale]
    result = [None, None]
    for step in range(NS_ITERS):
        for side in range(2):
            ys = halves(current[side])
            if step == 0:
                factor = 1.5 * eye - 0.5 * current[side]
                fs = halves(factor)
                result[side] = factor
            else:
                zs = halves(result[side])
                factor = 1.5 * eye - 0.5 * split_dot(zs, ys)
                fs = halves(factor)
                result[side] = split_dot(fs, zs)
            if step < NS_ITERS - 1:
                current[side] = split_dot(ys, fs)
    root = lax.sqrt(jnp.full((1, B), scale, F32))
    q1 = result[0] / root
    q2 = result[1] / root
    q1s, q2s = halves(q1), halves(q2)
    corner = split_dot(ks, q2s)
    lower = -split_dot(kts, q1s)
    for value, rows, cols in ((q1, 0, 0), (corner, 0, B), (lower, B, 0), (q2, B, B)):
        high, low = halves(value)
        wh_ref[rows : rows + B, cols : cols + B] = high
        wl_ref[rows : rows + B, cols : cols + B] = low
    lane = lax.broadcasted_iota(jnp.int32, (8, B), 1)
    own = STEPS * lax.axis_index("blk") + slot
    s_ref[...] = jnp.where(lane == own, squares, 0.0)


def roots(parts, slot):
    return pl.pallas_call(
        functools.partial(root_body, slot),
        in_specs=[VM] * 2,
        out_specs=[VM] * 3,
        out_shape=[
            jax.ShapeDtypeStruct((2 * B, 2 * B), BF16),
            jax.ShapeDtypeStruct((2 * B, 2 * B), BF16),
            jax.ShapeDtypeStruct((8, B), F32),
        ],
        compiler_params=params(8),
        cost_estimate=cost(30e6, 1e6),
    )(*parts)


def mixed(x, wh, wl):
    rows = x.shape[0]
    xh, xl = halves(x)
    both = dot(jnp.concatenate([xh, xl], axis=0), wh)
    return both[:rows] + (both[rows:] + dot(xh, wl))


def update_body(start, sizes, m_ref, wh_ref, wl_ref, *outs):
    wh, wl = wh_ref[...], wl_ref[...]
    at = start
    for n, size in enumerate(sizes):
        value = mixed(m_ref[at : at + size, :], wh, wl)
        outs[2 * n][...] = value[:, :B]
        outs[2 * n + 1][...] = value[:, B:]
        at += size


def update(matrix, w, start, sizes):
    shapes = []
    for size in sizes:
        shapes += [jax.ShapeDtypeStruct((size, B), F32)] * 2
    total = sum(sizes)
    outs = pl.pallas_call(
        functools.partial(update_body, start, tuple(sizes)),
        in_specs=[VM] * 3,
        out_specs=[VM] * len(shapes),
        out_shape=shapes,
        compiler_params=params(12),
        cost_estimate=cost(6 * total * 256 * 256, total * B * 16),
    )(matrix, *w)
    return outs[0::2], outs[1::2]


def partial_body(count, right_only, with_right, *refs):
    lefts = refs[:count]
    rights = refs[count : 2 * count]
    extra = refs[2 * count : 2 * count + right_only]
    o_ref = refs[-1]
    acc = jnp.zeros((B, B), F32)
    lsq = jnp.zeros((8, B), F32)
    rsq = jnp.zeros((8, B), F32)
    for left, right in zip(lefts, rights):
        x, y = left[...], right[...]
        acc = acc + gram_tile(x, y)
        lsq = lsq + column_squares(x)
        if with_right:
            rsq = rsq + column_squares(y)
    for right in extra:
        rsq = rsq + column_squares(right[...])
    tail = jnp.concatenate(
        [
            jnp.sum(lsq, axis=0, keepdims=True),
            jnp.sum(rsq, axis=0, keepdims=True),
            jnp.zeros((PACK - B - 2, B), F32),
        ],
        axis=0,
    )
    for base in refs[2 * count + right_only : -1]:
        acc = acc + base[:B, :]
        tail = tail + base[B:, :]
    o_ref[:B, :] = acc
    o_ref[B:, :] = tail


def partial(lefts, rights, extra, bases, with_right=True):
    total = sum(x.shape[0] for x in lefts)
    operands = [*lefts, *rights, *extra, *bases]
    return pl.pallas_call(
        functools.partial(partial_body, len(lefts), len(extra), with_right),
        in_specs=[VM] * len(operands),
        out_specs=VM,
        out_shape=jax.ShapeDtypeStruct((PACK, B), F32),
        compiler_params=params(12),
        cost_estimate=cost(total * B * B * 8, total * B * 8),
    )(*operands)


def second_body(rows0, aliased, count, joined, *refs):
    xs = refs[:count]
    others = refs[count : 2 * count] if joined else [None] * count
    refs = refs[count:] if joined else refs
    rs = refs[count : 2 * count]
    wh_ref, wl_ref = refs[2 * count : 2 * count + 2]
    rest = refs[2 * count + 2 + (1 if aliased else 0) :]
    out = rest[0]
    ys = rest[1 : 1 + count]
    held, sem = rest[1 + count :]
    wh, wl = wh_ref[...], wl_ref[...]
    at = 0
    for x, other, r, y in zip(xs, others, rs, ys):
        size = x.shape[0]
        left = x[...] if other is None else x[...] + other[...]
        value = mixed(jnp.concatenate([left, r[...]], axis=1), wh, wl)
        held[at : at + size, :] = value[:, :B]
        y[...] = value[:, B:]
        at += size
    copy = pltpu.make_async_copy(held, out.at[pl.ds(rows0, at), pl.ds(0, B)], sem)
    copy.start()
    copy.wait()


def second(xs, rs, w, out, rows, rows0, others=()):
    total = sum(x.shape[0] for x in xs)
    shapes = [jax.ShapeDtypeStruct((rows, 2 * B), F32)] + [
        jax.ShapeDtypeStruct(x.shape, F32) for x in xs
    ]
    operands = [*xs, *others, *rs, *w] + ([out] if out is not None else [])
    specs = [VM] * (2 * len(xs) + len(others) + 2) + ([HBM] if out is not None else [])
    return pl.pallas_call(
        functools.partial(second_body, rows0, out is not None, len(xs), bool(others)),
        in_specs=specs,
        out_specs=[HBM] + [VM] * len(xs),
        out_shape=shapes,
        scratch_shapes=[pltpu.VMEM((total, B), F32), pltpu.SemaphoreType.DMA],
        input_output_aliases={} if out is None else {len(operands) - 1: 0},
        compiler_params=params(12),
        cost_estimate=cost(6 * total * 256 * 256, total * B * 20),
    )(*operands)


def place_body(starts, *refs):
    count = len(starts)
    ys = refs[:count]
    out = refs[count + 1]
    sems = refs[count + 2]
    copies = []
    for n, (y, start) in enumerate(zip(ys, starts)):
        copies.append(
            pltpu.make_async_copy(
                y, out.at[pl.ds(start, y.shape[0]), pl.ds(B, B)], sems.at[n]
            )
        )
    for copy in copies:
        copy.start()
    for copy in copies:
        copy.wait()


def place(ys, starts, out):
    return pl.pallas_call(
        functools.partial(place_body, tuple(starts)),
        in_specs=[VM] * len(ys) + [HBM],
        out_specs=HBM,
        out_shape=jax.ShapeDtypeStruct(out.shape, F32),
        scratch_shapes=[pltpu.SemaphoreType.DMA((len(ys),))],
        input_output_aliases={len(ys): 0},
        compiler_params=params(8),
        cost_estimate=cost(1, sum(y.size for y in ys) * 8),
    )(*ys, out)


def shifted(value, steps, without=()):
    count = lax.axis_size("blk")
    routes = [(s, (s + steps) % count) for s in range(count) if s not in without]
    return lax.ppermute(value, "blk", routes)


def far_shifts():
    count = lax.axis_size("blk")
    plane = 32
    if count % plane:
        return {}
    ends = range(plane - 1, count, plane)
    return {s: (s - 3, (s + 2) % count, (s + 1) % count) for s in ends}


def relayed(value, leg):
    stops = [(s, *far) for s, far in far_shifts().items()]
    return lax.ppermute(value, "blk", [(t[leg], t[leg + 1]) for t in stops])


def of_group(value):
    count = lax.axis_size("row")

    def from_other(part, mask):
        return lax.ppermute(part, "row", [(s, s ^ mask) for s in range(count)])

    mask = 1
    while 2 * mask < count:
        value = value + from_other(value, mask)
        mask *= 2
    return value, from_other(value, mask)


def moved(value, where):
    count = lax.axis_size("blk")
    return lax.ppermute(value, "blk", [(s, where(s)) for s in range(count)])


def of_all_pairs(tile):
    count = lax.axis_size("blk")
    inner = 8 if count % 8 == 0 else count
    middle = 4 if count % (4 * inner) == 0 else 1
    outer = count // (inner * middle)

    def along_inner(steps):
        return lambda s: s // inner * inner + (s + steps) % inner

    def along_middle(steps):
        ring = inner * middle
        return lambda s: s // ring * ring + (s + steps * inner) % ring

    rounds = [[along_middle(-1)] for _ in range(1, middle)]
    reach = min(4, inner)
    rounds.append([along_inner(-n) for n in range(1, reach)])
    while reach < inner:
        step = min(3, inner - reach)
        rounds.append([along_inner(-step)])
        reach += step
    for n in range(1, outer):
        rounds.append([lambda s, n=n: (s + n * inner * middle) % count])
    for moves in rounds:
        for part in [moved(tile, where) for where in moves]:
            tile = jnp.maximum(tile, part)
    return tile


def mean_body(count, t_ref, o_ref):
    lane = lax.broadcasted_iota(jnp.int32, (1, B), 1)
    line = t_ref[0:1, :]
    for step in range(STEPS):
        own = (lane % STEPS == step) & (lane < STEPS * count)
        o_ref[step] = jnp.sum(jnp.where(own, line, 0.0)) / float(count)


def mean_over_pairs(tile):
    return pl.pallas_call(
        functools.partial(mean_body, lax.axis_size("blk")),
        in_specs=[VM],
        out_specs=pl.BlockSpec(memory_space=pltpu.SMEM),
        out_shape=jax.ShapeDtypeStruct((STEPS,), F32),
        compiler_params=params(4),
        cost_estimate=cost(1000, 1000),
        name="mean_over_pairs",
    )(tile)


def steps(matrix):
    rows = matrix.shape[0]
    unit = rows // UNITS
    front = [n * unit for n in FRONT]
    back = [n * unit for n in BACK]
    front_rows = sum(front)

    wh, wl, squares0 = roots(of_group(first_gram(matrix)), 0)
    w = (wh, wl)

    xf, rf = update(matrix, w, 0, front[:1])
    more_x, more_r = update(matrix, w, front[0], front[1:])
    xb, rb = update(matrix, w, front_rows, back)
    xf, rf = [*xf, *more_x], [*rf, *more_r]

    got = [shifted(x, 1) for x in xf]
    behind = [shifted(r, -1) for r in rb]
    helped = shifted(partial(xb, behind, [], [], False), 1)
    far = far_shifts()
    got_back = [shifted(x, 1, far) for x in xb]
    relays = xb[:RELAYED] if far else []
    for leg in range(3):
        relays = [relayed(x, leg) for x in relays]
    if far:
        near = set(range(lax.axis_size("blk"))) - set(far)
        relays += [shifted(x, 1, near) for x in xb[RELAYED:]]

    cut = len(got) - 1
    sums = partial(got[:cut], rf[:cut], rb, [])
    sums = partial(got[cut:], rf[cut:], [], [sums, helped])
    wh, wl, squares1 = roots(of_group(sums), 1)
    w = (wh, wl)

    out, *ys = second(got[:1], rf[:1], w, None, rows, 0)
    out, *more_y = second(got[1:], rf[1:], w, out, rows, front[0])
    out, *back_y = second(got_back, rb, w, out, rows, front_rows, relays)
    ys = [*ys, *more_y, *back_y]
    arrived = [shifted(y, 1) for y in ys]

    off_measure = mean_over_pairs(of_all_pairs(jnp.maximum(squares0, squares1)))
    places, at = [], 0
    for y in ys:
        places.append(at)
        at += y.shape[0]
    last = len(ys) - 1
    for lo, hi in ((0, last), (last, last + 1)):
        out = place(arrived[lo:hi], places[lo:hi], out)
    return out, off_measure


def solution(mesh):
    return jax.shard_map(
        steps,
        mesh=mesh,
        in_specs=(P("row", "blk"),),
        out_specs=(P("row", "blk"), P()),
        check_vma=False,
    )
```

```python
import functools

import jax
import jax.numpy as jnp
from jax import lax
from jax.experimental import pallas as pl
from jax.experimental.pallas import tpu as pltpu
from jax.sharding import PartitionSpec as P


STEPS = 2
NS_ITERS = 4
B = 128
PACK = 136
UNITS = 32
FRONT = (4, 16)
BACK = (8, 4)
RELAYED = 1

VM = pl.BlockSpec(memory_space=pltpu.VMEM)
ANY = pl.BlockSpec(memory_space=pl.ANY)
HBM = pl.BlockSpec(memory_space=pltpu.HBM)
F32 = jnp.float32
BF16 = jnp.bfloat16


def params(mib=24):
    return pltpu.CompilerParams(vmem_limit_bytes=mib * 1024 * 1024)


def cost(flops, moved):
    return pl.CostEstimate(flops=int(flops), bytes_accessed=int(moved), transcendentals=0)


def halves(x):
    high = x.astype(BF16)
    low = (x - high.astype(F32)).astype(BF16)
    return high, low


def dot(a, b):
    return jnp.dot(a, b, preferred_element_type=F32)


def dot_rows(a, b):
    return lax.dot_general(a, b, (((0,), (0,)), ((), ())), preferred_element_type=F32)


def split_dot(a, b):
    ah, al = a
    bh, bl = b
    return dot(ah, bh) + (dot(ah, bl) + dot(al, bh))


def gram_tile(left, right):
    lh, ll = halves(left)
    rh, rl = halves(right)
    full = dot_rows(jnp.concatenate([lh, ll], 1), jnp.concatenate([rh, rl], 1))
    return (full[:B, :B] + full[B:, B:]) + (full[:B, B:] + full[B:, :B])


def column_squares(x):
    return jnp.sum((x * x).reshape(x.shape[0] // 8, 8, x.shape[1]), axis=0)


def gram_body(blocks, m_ref, o_ref, held_ref, c_acc, n_acc, sems):
    block = m_ref.shape[0] // blocks

    def load(i):
        rows = pl.ds(i * block, block)
        return pltpu.make_async_copy(m_ref.at[rows, :], held_ref.at[rows, :], sems.at[i])

    for i in range(blocks):
        load(i).start()
    for i in range(blocks):
        load(i).wait()
        x = held_ref[i * block : (i + 1) * block, :]
        squares = column_squares(x)
        product = gram_tile(x[:, :B], x[:, B:])
        if i == 0:
            n_acc[...] = squares
            c_acc[...] = product
        else:
            n_acc[...] += squares
            c_acc[...] += product
    norms = jnp.sum(n_acc[...], axis=0, keepdims=True)
    o_ref[:B, :] = c_acc[...]
    o_ref[B:, :] = jnp.concatenate(
        [norms[:, :B], norms[:, B:], jnp.zeros((PACK - B - 2, B), F32)], axis=0
    )


def first_gram(matrix):
    rows = matrix.shape[0]
    return pl.pallas_call(
        functools.partial(gram_body, 8),
        in_specs=[HBM],
        out_specs=[VM, VM],
        out_shape=[
            jax.ShapeDtypeStruct((PACK, B), F32),
            jax.ShapeDtypeStruct(matrix.shape, F32),
        ],
        scratch_shapes=[
            pltpu.VMEM((B, B), F32),
            pltpu.VMEM((8, 2 * B), F32),
            pltpu.SemaphoreType.DMA((8,)),
        ],
        compiler_params=params(48),
        cost_estimate=cost(rows * B * B * 8, rows * B * 8),
        name="first_gram",
    )(matrix)


def root_body(slot, a_ref, b_ref, wh_ref, wl_ref, s_ref):
    total = a_ref[...] + b_ref[...]
    inverse = lax.rsqrt(total[B : B + 8, :])
    first = jnp.broadcast_to(inverse[0:1, :], (B, B)).T
    cosines = total[:B, :] * first * inverse[1:2, :]
    squares = jnp.sum(cosines * cosines)
    k = 0.5 * cosines
    scale = 1.0 + jnp.sum(k * k)
    kt = k.T
    row = lax.broadcasted_iota(jnp.int32, (B, B), 0)
    col = lax.broadcasted_iota(jnp.int32, (B, B), 1)
    eye = (row == col).astype(F32)
    ks, kts = halves(k), halves(kt)
    current = [(eye + split_dot(ks, kts)) / scale, (eye + split_dot(kts, ks)) / scale]
    result = [None, None]
    for step in range(NS_ITERS):
        for side in range(2):
            ys = halves(current[side])
            if step == 0:
                factor = 1.5 * eye - 0.5 * current[side]
                fs = halves(factor)
                result[side] = factor
            else:
                zs = halves(result[side])
                factor = 1.5 * eye - 0.5 * split_dot(zs, ys)
                fs = halves(factor)
                result[side] = split_dot(fs, zs)
            if step < NS_ITERS - 1:
                current[side] = split_dot(ys, fs)
    root = lax.sqrt(jnp.full((1, B), scale, F32))
    q1 = result[0] / root
    q2 = result[1] / root
    q1s, q2s = halves(q1), halves(q2)
    corner = split_dot(ks, q2s)
    lower = -split_dot(kts, q1s)
    for value, rows, cols in ((q1, 0, 0), (corner, 0, B), (lower, B, 0), (q2, B, B)):
        high, low = halves(value)
        wh_ref[rows : rows + B, cols : cols + B] = high
        wl_ref[rows : rows + B, cols : cols + B] = low
    lane = lax.broadcasted_iota(jnp.int32, (8, B), 1)
    own = STEPS * lax.axis_index("blk") + slot
    s_ref[...] = jnp.where(lane == own, squares, 0.0)


def roots(parts, slot):
    return pl.pallas_call(
        functools.partial(root_body, slot),
        in_specs=[VM] * 2,
        out_specs=[VM] * 3,
        out_shape=[
            jax.ShapeDtypeStruct((2 * B, 2 * B), BF16),
            jax.ShapeDtypeStruct((2 * B, 2 * B), BF16),
            jax.ShapeDtypeStruct((8, B), F32),
        ],
        compiler_params=params(8),
        cost_estimate=cost(30e6, 1e6),
    )(*parts)


def mixed(x, wh, wl):
    rows = x.shape[0]
    xh, xl = halves(x)
    both = dot(jnp.concatenate([xh, xl], axis=0), wh)
    return both[:rows] + (both[rows:] + dot(xh, wl))


def update_body(start, sizes, m_ref, wh_ref, wl_ref, *outs):
    wh, wl = wh_ref[...], wl_ref[...]
    at = start
    for n, size in enumerate(sizes):
        value = mixed(m_ref[at : at + size, :], wh, wl)
        outs[2 * n][...] = value[:, :B]
        outs[2 * n + 1][...] = value[:, B:]
        at += size


def update(matrix, w, start, sizes):
    shapes = []
    for size in sizes:
        shapes += [jax.ShapeDtypeStruct((size, B), F32)] * 2
    total = sum(sizes)
    outs = pl.pallas_call(
        functools.partial(update_body, start, tuple(sizes)),
        in_specs=[VM] * 3,
        out_specs=[VM] * len(shapes),
        out_shape=shapes,
        compiler_params=params(12),
        cost_estimate=cost(6 * total * 256 * 256, total * B * 16),
    )(matrix, *w)
    return outs[0::2], outs[1::2]


def partial_body(count, right_only, with_right, *refs):
    lefts = refs[:count]
    rights = refs[count : 2 * count]
    extra = refs[2 * count : 2 * count + right_only]
    o_ref = refs[-1]
    acc = jnp.zeros((B, B), F32)
    lsq = jnp.zeros((8, B), F32)
    rsq = jnp.zeros((8, B), F32)
    for left, right in zip(lefts, rights):
        x, y = left[...], right[...]
        acc = acc + gram_tile(x, y)
        lsq = lsq + column_squares(x)
        if with_right:
            rsq = rsq + column_squares(y)
    for right in extra:
        rsq = rsq + column_squares(right[...])
    tail = jnp.concatenate(
        [
            jnp.sum(lsq, axis=0, keepdims=True),
            jnp.sum(rsq, axis=0, keepdims=True),
            jnp.zeros((PACK - B - 2, B), F32),
        ],
        axis=0,
    )
    for base in refs[2 * count + right_only : -1]:
        acc = acc + base[:B, :]
        tail = tail + base[B:, :]
    o_ref[:B, :] = acc
    o_ref[B:, :] = tail


def partial(lefts, rights, extra, bases, with_right=True):
    total = sum(x.shape[0] for x in lefts)
    operands = [*lefts, *rights, *extra, *bases]
    return pl.pallas_call(
        functools.partial(partial_body, len(lefts), len(extra), with_right),
        in_specs=[VM] * len(operands),
        out_specs=VM,
        out_shape=jax.ShapeDtypeStruct((PACK, B), F32),
        compiler_params=params(12),
        cost_estimate=cost(total * B * B * 8, total * B * 8),
    )(*operands)


def second_body(rows0, aliased, count, joined, *refs):
    xs = refs[:count]
    others = refs[count : 2 * count] if joined else [None] * count
    refs = refs[count:] if joined else refs
    rs = refs[count : 2 * count]
    wh_ref, wl_ref = refs[2 * count : 2 * count + 2]
    rest = refs[2 * count + 2 + (1 if aliased else 0) :]
    out = rest[0]
    ys = rest[1 : 1 + count]
    held, sem = rest[1 + count :]
    wh, wl = wh_ref[...], wl_ref[...]
    at = 0
    for x, other, r, y in zip(xs, others, rs, ys):
        size = x.shape[0]
        left = x[...] if other is None else x[...] + other[...]
        value = mixed(jnp.concatenate([left, r[...]], axis=1), wh, wl)
        held[at : at + size, :] = value[:, :B]
        y[...] = value[:, B:]
        at += size
    copy = pltpu.make_async_copy(held, out.at[pl.ds(rows0, at), pl.ds(0, B)], sem)
    copy.start()
    copy.wait()


def second(xs, rs, w, out, rows, rows0, others=()):
    total = sum(x.shape[0] for x in xs)
    shapes = [jax.ShapeDtypeStruct((rows, 2 * B), F32)] + [
        jax.ShapeDtypeStruct(x.shape, F32) for x in xs
    ]
    operands = [*xs, *others, *rs, *w] + ([out] if out is not None else [])
    specs = [VM] * (2 * len(xs) + len(others) + 2) + ([HBM] if out is not None else [])
    return pl.pallas_call(
        functools.partial(second_body, rows0, out is not None, len(xs), bool(others)),
        in_specs=specs,
        out_specs=[HBM] + [VM] * len(xs),
        out_shape=shapes,
        scratch_shapes=[pltpu.VMEM((total, B), F32), pltpu.SemaphoreType.DMA],
        input_output_aliases={} if out is None else {len(operands) - 1: 0},
        compiler_params=params(12),
        cost_estimate=cost(6 * total * 256 * 256, total * B * 20),
    )(*operands)


def place_body(starts, *refs):
    count = len(starts)
    ys = refs[:count]
    out = refs[count + 1]
    sems = refs[count + 2]
    copies = []
    for n, (y, start) in enumerate(zip(ys, starts)):
        copies.append(
            pltpu.make_async_copy(
                y, out.at[pl.ds(start, y.shape[0]), pl.ds(B, B)], sems.at[n]
            )
        )
    for copy in copies:
        copy.start()
    for copy in copies:
        copy.wait()


def place(ys, starts, out):
    return pl.pallas_call(
        functools.partial(place_body, tuple(starts)),
        in_specs=[VM] * len(ys) + [HBM],
        out_specs=HBM,
        out_shape=jax.ShapeDtypeStruct(out.shape, F32),
        scratch_shapes=[pltpu.SemaphoreType.DMA((len(ys),))],
        input_output_aliases={len(ys): 0},
        compiler_params=params(8),
        cost_estimate=cost(1, sum(y.size for y in ys) * 8),
    )(*ys, out)


def shifted(value, steps, without=()):
    count = lax.axis_size("blk")
    routes = [(s, (s + steps) % count) for s in range(count) if s not in without]
    return lax.ppermute(value, "blk", routes)


def far_shifts():
    count = lax.axis_size("blk")
    plane = 32
    if count % plane:
        return {}
    ends = range(plane - 1, count, plane)
    return {s: (s - 3, (s + 2) % count, (s + 1) % count) for s in ends}


def relayed(value, leg):
    stops = [(s, *far) for s, far in far_shifts().items()]
    return lax.ppermute(value, "blk", [(t[leg], t[leg + 1]) for t in stops])


def of_group(value):
    count = lax.axis_size("row")

    def from_other(part, mask):
        return lax.ppermute(part, "row", [(s, s ^ mask) for s in range(count)])

    mask = 1
    while 2 * mask < count:
        value = value + from_other(value, mask)
        mask *= 2
    return value, from_other(value, mask)


def moved(value, where):
    count = lax.axis_size("blk")
    return lax.ppermute(value, "blk", [(s, where(s)) for s in range(count)])


def of_all_pairs(tile):
    count = lax.axis_size("blk")
    inner = 8 if count % 8 == 0 else count
    middle = 4 if count % (4 * inner) == 0 else 1
    outer = count // (inner * middle)

    def along_inner(steps):
        return lambda s: s // inner * inner + (s + steps) % inner

    def along_middle(steps):
        ring = inner * middle
        return lambda s: s // ring * ring + (s + steps * inner) % ring

    rounds = [[along_middle(-1)] for _ in range(1, middle)]
    reach = min(4, inner)
    rounds.append([along_inner(-n) for n in range(1, reach)])
    while reach < inner:
        step = min(3, inner - reach)
        rounds.append([along_inner(-step)])
        reach += step
    for n in range(1, outer):
        rounds.append([lambda s, n=n: (s + n * inner * middle) % count])
    for moves in rounds:
        for part in [moved(tile, where) for where in moves]:
            tile = jnp.maximum(tile, part)
    return tile


def mean_body(count, t_ref, o_ref):
    lane = lax.broadcasted_iota(jnp.int32, (1, B), 1)
    line = t_ref[0:1, :]
    for step in range(STEPS):
        own = (lane % STEPS == step) & (lane < STEPS * count)
        o_ref[step] = jnp.sum(jnp.where(own, line, 0.0)) / float(count)


def mean_over_pairs(tile):
    return pl.pallas_call(
        functools.partial(mean_body, lax.axis_size("blk")),
        in_specs=[VM],
        out_specs=pl.BlockSpec(memory_space=pltpu.SMEM),
        out_shape=jax.ShapeDtypeStruct((STEPS,), F32),
        compiler_params=params(4),
        cost_estimate=cost(1000, 1000),
        name="mean_over_pairs",
    )(tile)


def steps(matrix):
    rows = matrix.shape[0]
    unit = rows // UNITS
    front = [n * unit for n in FRONT]
    back = [n * unit for n in BACK]
    front_rows = sum(front)

    sums, matrix = first_gram(matrix)
    wh, wl, squares0 = roots(of_group(sums), 0)
    w = (wh, wl)

    xf, rf = update(matrix, w, 0, front[:1])
    more_x, more_r = update(matrix, w, front[0], front[1:])
    xb, rb = update(matrix, w, front_rows, back)
    xf, rf = [*xf, *more_x], [*rf, *more_r]

    got = [shifted(x, 1) for x in xf]
    behind = [shifted(r, -1) for r in rb]
    helped = shifted(partial(xb, behind, [], [], False), 1)
    far = far_shifts()
    got_back = [shifted(x, 1, far) for x in xb]
    relays = xb[:RELAYED] if far else []
    for leg in range(3):
        relays = [relayed(x, leg) for x in relays]
    if far:
        near = set(range(lax.axis_size("blk"))) - set(far)
        relays += [shifted(x, 1, near) for x in xb[RELAYED:]]

    cut = len(got) - 1
    sums = partial(got[:cut], rf[:cut], rb, [])
    sums = partial(got[cut:], rf[cut:], [], [sums, helped])
    wh, wl, squares1 = roots(of_group(sums), 1)
    w = (wh, wl)

    out, *ys = second(got[:1], rf[:1], w, None, rows, 0)
    out, *more_y = second(got[1:], rf[1:], w, out, rows, front[0])
    out, *back_y = second(got_back, rb, w, out, rows, front_rows, relays)
    ys = [*ys, *more_y, *back_y]
    arrived = [shifted(y, 1) for y in ys]

    off_measure = mean_over_pairs(of_all_pairs(jnp.maximum(squares0, squares1)))
    places, at = [], 0
    for y in ys:
        places.append(at)
        at += y.shape[0]
    last = len(ys) - 1
    for lo, hi in ((0, last), (last, last + 1)):
        out = place(arrived[lo:hi], places[lo:hi], out)
    return out, off_measure


def solution(mesh):
    return jax.shard_map(
        steps,
        mesh=mesh,
        in_specs=(P("row", "blk"),),
        out_specs=(P("row", "blk"), P()),
        check_vma=False,
    )
```

```python
import functools

import jax
import jax.numpy as jnp
from jax import lax
from jax.experimental import pallas as pl
from jax.experimental.pallas import tpu as pltpu
from jax.sharding import PartitionSpec as P


STEPS = 2
NS_ITERS = 4
B = 128
PACK = 136
UNITS = 32
FRONT = (4, 16)
BACK = (8, 4)
RELAYED = 1

VM = pl.BlockSpec(memory_space=pltpu.VMEM)
ANY = pl.BlockSpec(memory_space=pl.ANY)
HBM = pl.BlockSpec(memory_space=pltpu.HBM)
F32 = jnp.float32
BF16 = jnp.bfloat16


def params(mib=24):
    return pltpu.CompilerParams(vmem_limit_bytes=mib * 1024 * 1024)


def cost(flops, moved):
    return pl.CostEstimate(flops=int(flops), bytes_accessed=int(moved), transcendentals=0)


def halves(x):
    high = x.astype(BF16)
    low = (x - high.astype(F32)).astype(BF16)
    return high, low


def dot(a, b):
    return jnp.dot(a, b, preferred_element_type=F32)


def dot_rows(a, b):
    return lax.dot_general(a, b, (((0,), (0,)), ((), ())), preferred_element_type=F32)


def split_dot(a, b):
    ah, al = a
    bh, bl = b
    return dot(ah, bh) + (dot(ah, bl) + dot(al, bh))


def gram_tile(left, right):
    lh, ll = halves(left)
    rh, rl = halves(right)
    full = dot_rows(jnp.concatenate([lh, ll], 1), jnp.concatenate([rh, rl], 1))
    return (full[:B, :B] + full[B:, B:]) + (full[:B, B:] + full[B:, :B])


def column_squares(x):
    return jnp.sum((x * x).reshape(x.shape[0] // 8, 8, x.shape[1]), axis=0)


def gram_body(blocks, m_ref, o_ref, held_ref, c_acc, n_acc, sems):
    block = m_ref.shape[0] // blocks

    def load(i):
        rows = pl.ds(i * block, block)
        return pltpu.make_async_copy(m_ref.at[rows, :], held_ref.at[rows, :], sems.at[i])

    for i in range(blocks):
        load(i).start()
    for i in range(blocks):
        load(i).wait()
        x = held_ref[i * block : (i + 1) * block, :]
        squares = column_squares(x)
        high, low = halves(x)
        product = dot_rows(
            jnp.concatenate([high[:, :B], low[:, :B]], 1),
            jnp.concatenate([high[:, B:], low[:, B:]], 1),
        )
        if i == 0:
            n_acc[...] = squares
            c_acc[...] = product
        else:
            n_acc[...] += squares
            c_acc[...] += product
    full = c_acc[...]
    norms = jnp.sum(n_acc[...], axis=0, keepdims=True)
    o_ref[:B, :] = (full[:B, :B] + full[B:, B:]) + (full[:B, B:] + full[B:, :B])
    o_ref[B:, :] = jnp.concatenate(
        [norms[:, :B], norms[:, B:], jnp.zeros((PACK - B - 2, B), F32)], axis=0
    )


def first_gram(matrix):
    rows = matrix.shape[0]
    return pl.pallas_call(
        functools.partial(gram_body, 4),
        in_specs=[HBM],
        out_specs=[VM, VM],
        out_shape=[
            jax.ShapeDtypeStruct((PACK, B), F32),
            jax.ShapeDtypeStruct(matrix.shape, F32),
        ],
        scratch_shapes=[
            pltpu.VMEM((2 * B, 2 * B), F32),
            pltpu.VMEM((8, 2 * B), F32),
            pltpu.SemaphoreType.DMA((4,)),
        ],
        compiler_params=params(48),
        cost_estimate=cost(rows * B * B * 8, rows * B * 8),
        name="first_gram",
    )(matrix)


def root_body(slot, a_ref, b_ref, wh_ref, wl_ref, s_ref):
    total = a_ref[...] + b_ref[...]
    inverse = lax.rsqrt(total[B : B + 8, :])
    first = jnp.broadcast_to(inverse[0:1, :], (B, B)).T
    cosines = total[:B, :] * first * inverse[1:2, :]
    squares = jnp.sum(cosines * cosines)
    k = 0.5 * cosines
    scale = 1.0 + jnp.sum(k * k)
    kt = k.T
    row = lax.broadcasted_iota(jnp.int32, (B, B), 0)
    col = lax.broadcasted_iota(jnp.int32, (B, B), 1)
    eye = (row == col).astype(F32)
    ks, kts = halves(k), halves(kt)
    current = [(eye + split_dot(ks, kts)) / scale, (eye + split_dot(kts, ks)) / scale]
    result = [None, None]
    for step in range(NS_ITERS):
        for side in range(2):
            ys = halves(current[side])
            if step == 0:
                factor = 1.5 * eye - 0.5 * current[side]
                fs = halves(factor)
                result[side] = factor
            else:
                zs = halves(result[side])
                factor = 1.5 * eye - 0.5 * split_dot(zs, ys)
                fs = halves(factor)
                result[side] = split_dot(fs, zs)
            if step < NS_ITERS - 1:
                current[side] = split_dot(ys, fs)
    root = lax.sqrt(jnp.full((1, B), scale, F32))
    q1 = result[0] / root
    q2 = result[1] / root
    q1s, q2s = halves(q1), halves(q2)
    corner = split_dot(ks, q2s)
    lower = -split_dot(kts, q1s)
    for value, rows, cols in ((q1, 0, 0), (corner, 0, B), (lower, B, 0), (q2, B, B)):
        high, low = halves(value)
        wh_ref[rows : rows + B, cols : cols + B] = high
        wl_ref[rows : rows + B, cols : cols + B] = low
    lane = lax.broadcasted_iota(jnp.int32, (8, B), 1)
    own = STEPS * lax.axis_index("blk") + slot
    s_ref[...] = jnp.where(lane == own, squares, 0.0)


def roots(parts, slot):
    return pl.pallas_call(
        functools.partial(root_body, slot),
        in_specs=[VM] * 2,
        out_specs=[VM] * 3,
        out_shape=[
            jax.ShapeDtypeStruct((2 * B, 2 * B), BF16),
            jax.ShapeDtypeStruct((2 * B, 2 * B), BF16),
            jax.ShapeDtypeStruct((8, B), F32),
        ],
        compiler_params=params(8),
        cost_estimate=cost(30e6, 1e6),
    )(*parts)


def mixed(x, wh, wl):
    rows = x.shape[0]
    xh, xl = halves(x)
    both = dot(jnp.concatenate([xh, xl], axis=0), wh)
    return both[:rows] + (both[rows:] + dot(xh, wl))


def update_body(start, sizes, m_ref, wh_ref, wl_ref, *outs):
    wh, wl = wh_ref[...], wl_ref[...]
    at = start
    for n, size in enumerate(sizes):
        value = mixed(m_ref[at : at + size, :], wh, wl)
        outs[2 * n][...] = value[:, :B]
        outs[2 * n + 1][...] = value[:, B:]
        at += size


def update(matrix, w, start, sizes):
    shapes = []
    for size in sizes:
        shapes += [jax.ShapeDtypeStruct((size, B), F32)] * 2
    total = sum(sizes)
    outs = pl.pallas_call(
        functools.partial(update_body, start, tuple(sizes)),
        in_specs=[VM] * 3,
        out_specs=[VM] * len(shapes),
        out_shape=shapes,
        compiler_params=params(12),
        cost_estimate=cost(6 * total * 256 * 256, total * B * 16),
    )(matrix, *w)
    return outs[0::2], outs[1::2]


def partial_body(count, right_only, with_right, *refs):
    lefts = refs[:count]
    rights = refs[count : 2 * count]
    extra = refs[2 * count : 2 * count + right_only]
    o_ref = refs[-1]
    acc = jnp.zeros((B, B), F32)
    lsq = jnp.zeros((8, B), F32)
    rsq = jnp.zeros((8, B), F32)
    for left, right in zip(lefts, rights):
        x, y = left[...], right[...]
        acc = acc + gram_tile(x, y)
        lsq = lsq + column_squares(x)
        if with_right:
            rsq = rsq + column_squares(y)
    for right in extra:
        rsq = rsq + column_squares(right[...])
    tail = jnp.concatenate(
        [
            jnp.sum(lsq, axis=0, keepdims=True),
            jnp.sum(rsq, axis=0, keepdims=True),
            jnp.zeros((PACK - B - 2, B), F32),
        ],
        axis=0,
    )
    for base in refs[2 * count + right_only : -1]:
        acc = acc + base[:B, :]
        tail = tail + base[B:, :]
    o_ref[:B, :] = acc
    o_ref[B:, :] = tail


def partial(lefts, rights, extra, bases, with_right=True):
    total = sum(x.shape[0] for x in lefts)
    operands = [*lefts, *rights, *extra, *bases]
    return pl.pallas_call(
        functools.partial(partial_body, len(lefts), len(extra), with_right),
        in_specs=[VM] * len(operands),
        out_specs=VM,
        out_shape=jax.ShapeDtypeStruct((PACK, B), F32),
        compiler_params=params(12),
        cost_estimate=cost(total * B * B * 8, total * B * 8),
    )(*operands)


def second_body(rows0, aliased, count, joined, *refs):
    xs = refs[:count]
    others = refs[count : 2 * count] if joined else [None] * count
    refs = refs[count:] if joined else refs
    rs = refs[count : 2 * count]
    wh_ref, wl_ref = refs[2 * count : 2 * count + 2]
    rest = refs[2 * count + 2 + (1 if aliased else 0) :]
    out = rest[0]
    ys = rest[1 : 1 + count]
    held, sem = rest[1 + count :]
    wh, wl = wh_ref[...], wl_ref[...]
    at = 0
    for x, other, r, y in zip(xs, others, rs, ys):
        size = x.shape[0]
        left = x[...] if other is None else x[...] + other[...]
        value = mixed(jnp.concatenate([left, r[...]], axis=1), wh, wl)
        held[at : at + size, :] = value[:, :B]
        y[...] = value[:, B:]
        at += size
    copy = pltpu.make_async_copy(held, out.at[pl.ds(rows0, at), pl.ds(0, B)], sem)
    copy.start()
    copy.wait()


def second(xs, rs, w, out, rows, rows0, others=()):
    total = sum(x.shape[0] for x in xs)
    shapes = [jax.ShapeDtypeStruct((rows, 2 * B), F32)] + [
        jax.ShapeDtypeStruct(x.shape, F32) for x in xs
    ]
    operands = [*xs, *others, *rs, *w] + ([out] if out is not None else [])
    specs = [VM] * (2 * len(xs) + len(others) + 2) + ([HBM] if out is not None else [])
    return pl.pallas_call(
        functools.partial(second_body, rows0, out is not None, len(xs), bool(others)),
        in_specs=specs,
        out_specs=[HBM] + [VM] * len(xs),
        out_shape=shapes,
        scratch_shapes=[pltpu.VMEM((total, B), F32), pltpu.SemaphoreType.DMA],
        input_output_aliases={} if out is None else {len(operands) - 1: 0},
        compiler_params=params(12),
        cost_estimate=cost(6 * total * 256 * 256, total * B * 20),
    )(*operands)


def place_body(starts, *refs):
    count = len(starts)
    ys = refs[:count]
    out = refs[count + 1]
    sems = refs[count + 2]
    copies = []
    for n, (y, start) in enumerate(zip(ys, starts)):
        copies.append(
            pltpu.make_async_copy(
                y, out.at[pl.ds(start, y.shape[0]), pl.ds(B, B)], sems.at[n]
            )
        )
    for copy in copies:
        copy.start()
    for copy in copies:
        copy.wait()


def place(ys, starts, out):
    return pl.pallas_call(
        functools.partial(place_body, tuple(starts)),
        in_specs=[VM] * len(ys) + [HBM],
        out_specs=HBM,
        out_shape=jax.ShapeDtypeStruct(out.shape, F32),
        scratch_shapes=[pltpu.SemaphoreType.DMA((len(ys),))],
        input_output_aliases={len(ys): 0},
        compiler_params=params(8),
        cost_estimate=cost(1, sum(y.size for y in ys) * 8),
    )(*ys, out)


def shifted(value, steps, without=()):
    count = lax.axis_size("blk")
    routes = [(s, (s + steps) % count) for s in range(count) if s not in without]
    return lax.ppermute(value, "blk", routes)


def far_shifts():
    count = lax.axis_size("blk")
    plane = 32
    if count % plane:
        return {}
    ends = range(plane - 1, count, plane)
    return {s: (s - 3, (s + 2) % count, (s + 1) % count) for s in ends}


def relayed(value, leg):
    stops = [(s, *far) for s, far in far_shifts().items()]
    return lax.ppermute(value, "blk", [(t[leg], t[leg + 1]) for t in stops])


def of_group(value):
    count = lax.axis_size("row")

    def from_other(part, mask):
        return lax.ppermute(part, "row", [(s, s ^ mask) for s in range(count)])

    mask = 1
    while 2 * mask < count:
        value = value + from_other(value, mask)
        mask *= 2
    return value, from_other(value, mask)


def moved(value, where):
    count = lax.axis_size("blk")
    return lax.ppermute(value, "blk", [(s, where(s)) for s in range(count)])


def of_all_pairs(tile):
    count = lax.axis_size("blk")
    inner = 8 if count % 8 == 0 else count
    middle = 4 if count % (4 * inner) == 0 else 1
    outer = count // (inner * middle)

    def along_inner(steps):
        return lambda s: s // inner * inner + (s + steps) % inner

    def along_middle(steps):
        ring = inner * middle
        return lambda s: s // ring * ring + (s + steps * inner) % ring

    rounds = [[along_middle(-1)] for _ in range(1, middle)]
    reach = min(4, inner)
    rounds.append([along_inner(-n) for n in range(1, reach)])
    while reach < inner:
        step = min(3, inner - reach)
        rounds.append([along_inner(-step)])
        reach += step
    for n in range(1, outer):
        rounds.append([lambda s, n=n: (s + n * inner * middle) % count])
    for moves in rounds:
        for part in [moved(tile, where) for where in moves]:
            tile = jnp.maximum(tile, part)
    return tile


def mean_body(count, t_ref, o_ref):
    lane = lax.broadcasted_iota(jnp.int32, (1, B), 1)
    line = t_ref[0:1, :]
    for step in range(STEPS):
        own = (lane % STEPS == step) & (lane < STEPS * count)
        o_ref[step] = jnp.sum(jnp.where(own, line, 0.0)) / float(count)


def mean_over_pairs(tile):
    return pl.pallas_call(
        functools.partial(mean_body, lax.axis_size("blk")),
        in_specs=[VM],
        out_specs=pl.BlockSpec(memory_space=pltpu.SMEM),
        out_shape=jax.ShapeDtypeStruct((STEPS,), F32),
        compiler_params=params(4),
        cost_estimate=cost(1000, 1000),
        name="mean_over_pairs",
    )(tile)


def steps(matrix):
    rows = matrix.shape[0]
    unit = rows // UNITS
    front = [n * unit for n in FRONT]
    back = [n * unit for n in BACK]
    front_rows = sum(front)

    sums, matrix = first_gram(matrix)
    wh, wl, squares0 = roots(of_group(sums), 0)
    w = (wh, wl)

    xf, rf = update(matrix, w, 0, front[:1])
    more_x, more_r = update(matrix, w, front[0], front[1:])
    xb, rb = update(matrix, w, front_rows, back)
    xf, rf = [*xf, *more_x], [*rf, *more_r]

    got = [shifted(x, 1) for x in xf]
    behind = [shifted(r, -1) for r in rb]
    helped = shifted(partial(xb, behind, [], [], False), 1)
    far = far_shifts()
    got_back = [shifted(x, 1, far) for x in xb]
    relays = xb[:RELAYED] if far else []
    for leg in range(3):
        relays = [relayed(x, leg) for x in relays]
    if far:
        near = set(range(lax.axis_size("blk"))) - set(far)
        relays += [shifted(x, 1, near) for x in xb[RELAYED:]]

    cut = len(got) - 1
    sums = partial(got[:cut], rf[:cut], rb, [])
    sums = partial(got[cut:], rf[cut:], [], [sums]) + helped
    wh, wl, squares1 = roots(of_group(sums), 1)
    w = (wh, wl)

    out, *ys = second(got[:1], rf[:1], w, None, rows, 0)
    out, *more_y = second(got[1:], rf[1:], w, out, rows, front[0])
    out, *back_y = second(got_back, rb, w, out, rows, front_rows, relays)
    ys = [*ys, *more_y, *back_y]
    arrived = [shifted(y, 1) for y in ys]

    off_measure = mean_over_pairs(of_all_pairs(jnp.maximum(squares0, squares1)))
    places, at = [], 0
    for y in ys:
        places.append(at)
        at += y.shape[0]
    last = len(ys) - 1
    for lo, hi in ((0, last), (last, last + 1)):
        out = place(arrived[lo:hi], places[lo:hi], out)
    return out, off_measure


def solution(mesh):
    return jax.shard_map(
        steps,
        mesh=mesh,
        in_specs=(P("row", "blk"),),
        out_specs=(P("row", "blk"), P()),
        check_vma=False,
    )
```
